256 devices in a mesh: grp: 8 (over x_lo, y), smp: 32 (over x_hi, z, core).
Axes of the slice: x: 4 (x_hi: 2, x_lo: 2; x = x_hi * 2 + x_lo), y: 4, z: 8, core: 2. Of those that a mesh axis runs over, the one named last changes fastest.
Arguments:
- spins_packed: int32 [32, 32768], P(None, 'smp'), may hold values from -2147483648 to 2147483646
- weight: bfloat16 [1024, 8192], P(None, 'grp'), may hold values from -0.1875 to 0.1875
- hidden_bias: float32 [8192], P('grp'), may hold values from -1.5 to 1.5
- force_w: float32 [1024, 8192], P('smp', 'grp'), may hold values from -6 to 6
- force_b: float32 [8192], P('grp'), may hold values from -6 to 6
Outputs:
- update_w: float32 [1024, 8192], P('smp', 'grp')
- update_b: float32 [8192], P('grp')
The draws below stay inside these ranges and needn't reach their ends.
All inputs are finite; a program needn't handle non-finite values.
Results may differ from the reference program's by a relative error of at most 0.0003.
Values sent between devices are 32-bit elements; how exact they have to be, the bound alone decides.
A program may use at most 64 MiB of HBM per device.

```python
import jax
import jax.numpy as jnp
from jax import lax

NV = 1024
NH = 8192
TOK_DEV = 1024
ITERS = 2
WORDS = 32
TOKENS = 32768


def with_ends(entries, stream_key, low, high):
    dims = entries.shape
    spot = [jax.random.randint(jax.random.fold_in(stream_key, axis), (), 0, dims[axis]) for axis in range(len(dims))]
    entries = entries.at[tuple(spot)].set(low)
    longest = dims.index(max(dims))
    spot[longest] = (spot[longest] + 1) % dims[longest]
    return entries.at[tuple(spot)].set(high)


def block_levels(stream_key, dims, split, smallest, top_value):
    level = 1.0
    for axis_at, shards_of in split:
        heights = jax.random.uniform(jax.random.fold_in(jax.random.fold_in(stream_key, 6), axis_at), (shards_of,), jnp.float32, smallest / len(split), top_value / len(split))
        level = level * jnp.repeat(jnp.exp(heights), dims[axis_at] // shards_of).reshape((-1,) + (1,) * (len(dims) - 1 - axis_at))
    return level


def bell_draw(rng, shape, width, reach, shards=(), kind=jnp.bfloat16):
    array = width * jax.random.normal(rng, shape, jnp.float32)
    if shards:
        array = array * block_levels(rng, shape, shards, -0.22, 0.18)
    return jnp.clip(array, -reach, reach).astype(kind)


def setup_inputs(seed: int = 0) -> dict:
    key_of = jax.random.split(jax.random.key(seed), 6)
    spins_packed = with_ends(jax.random.randint(key_of[0], (WORDS, TOKENS), -2147483648, 2147483647), jax.random.fold_in(key_of[0], 1), -2147483648, 2147483646).astype(jnp.int32)
    weight = bell_draw(key_of[1], (NV, NH), NV ** -0.5, 0.1875, ((1, 8),))
    hidden_bias = jnp.clip(jax.random.uniform(key_of[2], (NH,), jnp.float32, -1.5, 1.5) * block_levels(key_of[2], (NH,), ((0, 8),), -0.4, 0.0), -1.5, 1.5)
    force_w = bell_draw(key_of[3], (NV, NH), 1.0, 6.0, ((0, 32), (1, 8)), jnp.float32)
    force_b = bell_draw(key_of[4], (NH,), 1.0, 6.0, ((0, 8),), jnp.float32)
    return dict(spins_packed=spins_packed, weight=weight, hidden_bias=hidden_bias, force_w=force_w, force_b=force_b)


diag_shift = 0.01


def unpack(packed):
    shifts = jnp.arange(32, dtype=jnp.int32)
    bit_values = jnp.bitwise_and(jnp.right_shift(packed[:, None, :], shifts[None, :, None]), 1)
    signs = 2 * bit_values - 1
    return signs.reshape(packed.shape[0] * 32, packed.shape[1]).astype(jnp.bfloat16)


def reference(spins_packed, weight, hidden_bias, force_w, force_b):
    spins = unpack(spins_packed)
    tile_count = TOKENS // TOK_DEV
    tiles = spins.reshape(NV, tile_count, TOK_DEV).transpose(1, 0, 2)

    def activations(sample_tile):
        pre_activation = jnp.einsum("it,ih->th", sample_tile, weight, preferred_element_type=jnp.float32)
        return jnp.tanh(pre_activation + hidden_bias)

    def forward(direction_w, direction_b):
        def scan_step(running, sample_tile):
            hidden = activations(sample_tile)
            projected = jnp.einsum("it,ih->th", sample_tile, direction_w, precision=lax.Precision.HIGHEST, preferred_element_type=jnp.float32)
            return running, jnp.sum(hidden * (projected + direction_b), axis=1)

        _, sample_values = lax.scan(scan_step, jnp.zeros((), jnp.float32), tiles)
        sample_values = sample_values.reshape(TOKENS)
        return sample_values - jnp.sum(sample_values) / TOKENS

    def metric(centred, direction_w, direction_b):
        scaled = (centred / TOKENS).reshape(tile_count, TOK_DEV)

        def scan_step(running, inputs):
            sample_tile, weights_now = inputs
            hidden = activations(sample_tile)
            weighted = weights_now[:, None] * hidden
            grad_w = running[0] + jnp.einsum("it,th->ih", sample_tile, weighted, precision=lax.Precision.HIGHEST, preferred_element_type=jnp.float32)
            grad_b = running[1] + jnp.dot(weights_now, hidden, precision=lax.Precision.HIGHEST, preferred_element_type=jnp.float32)
            return (grad_w, grad_b), None

        zeros_pair = (jnp.zeros((NV, NH), jnp.float32), jnp.zeros((NH,), jnp.float32))
        (grad_w, grad_b), _ = lax.scan(scan_step, zeros_pair, (tiles, scaled))
        return grad_w + diag_shift * direction_w, grad_b + diag_shift * direction_b

    solution_w = jnp.zeros_like(force_w)
    solution_b = jnp.zeros_like(force_b)
    residual_w, residual_b = force_w, force_b
    direction_w, direction_b = force_w, force_b
    norm_now = jnp.sum(residual_w * residual_w) + jnp.sum(residual_b * residual_b)
    for iteration in range(ITERS):
        centred = forward(direction_w, direction_b)
        curvature = jnp.sum(centred * centred) / TOKENS + diag_shift * (jnp.sum(direction_w * direction_w) + jnp.sum(direction_b * direction_b))
        step_size = norm_now / curvature
        solution_w = solution_w + step_size * direction_w
        solution_b = solution_b + step_size * direction_b
        if iteration + 1 < ITERS:
            image_w, image_b = metric(centred, direction_w, direction_b)
            residual_w = residual_w - step_size * image_w
            residual_b = residual_b - step_size * image_b
            norm_next = jnp.sum(residual_w * residual_w) + jnp.sum(residual_b * residual_b)
            direction_w = residual_w + (norm_next / norm_now) * direction_w
            direction_b = residual_b + (norm_next / norm_now) * direction_b
            norm_now = norm_next
    return solution_w, solution_b
```

```python
import functools

import jax
import jax.numpy as jnp
from jax import lax
from jax.experimental import pallas as pl
from jax.experimental.pallas import tpu as pltpu
from jax.sharding import PartitionSpec as P

MESH = pl.DeviceIdType.MESH
LAMBDA = 0.01
F32 = jnp.float32
BF16 = jnp.bfloat16
LANES = 128


def split(x):
    hi = x.astype(BF16)
    return hi, (x - hi.astype(F32)).astype(BF16)


def folded(x):
    rows, cols = x.shape
    tiles = [x[r : r + 8, k : k + LANES] for r in range(0, rows, 8) for k in range(0, cols, LANES)]
    return functools.reduce(lambda a, b: a + b, tiles)


def total(x):
    return jnp.sum(jnp.sum(x, axis=0, keepdims=True), axis=1, keepdims=True)


def kernel(ng, nz, count, spk, w_hbm, hb, fw, fb, out_w, out_b,
           pk, wv, wt, fc, ft, sgn, hid, ch, acc, vbuf, v1, s2, r2, s3, r3, x1s, x1, x2s, x2,
           w1, s4, r4, s5, r5, gb, rs_s, rs_r, gall, gown, cols,
           local_sem, send, pk_sem, fa_sem, fx_sem, v1_sem, v2_sem, v3_sem, x1_sem, x2_sem, w1_sem, w2_sem, w3_sem,
           rs_sem, ag_sem, gz_sem):
    ns = 4 * nz
    rows = 8 * ns
    tok = spk.shape[1]
    tiles = tok // LANES
    s = lax.axis_index("smp")
    g = lax.axis_index("grp")
    xh = s // (2 * nz)
    z = (s // 2) % nz
    c = s % 2
    q_me = 2 * xh + c
    q_core = 2 * xh + 1 - c
    q_x = 2 * (1 - xh) + c
    q_far = 2 * (1 - xh) + 1 - c
    core = s + 1 - 2 * c
    across = s + (2 * nz) * (1 - 2 * xh)

    def z_index(k):
        return 2 * nz * xh + 2 * k + c

    def remote(src, dst, ssem, rsem, dev):
        return pltpu.make_async_remote_copy(src_ref=src, dst_ref=dst, send_sem=ssem, recv_sem=rsem,
                                            device_id=dev, device_id_type=MESH)

    def peers(n, me, act):
        def step(j, carry):
            act(lax.rem(me + j, n))
            return carry
        lax.fori_loop(1, n, step, 0)

    class Exchange:
        def __init__(self, n, me, dev, src, dst, number, sems):
            self.n, self.me, self.dev, self.src, self.dst = n, me, dev, src, dst
            self.ssem, self.sems = send.at[number], sems

        def copy(self, peer, slot):
            return remote(self.src(peer), self.dst(slot), self.ssem, self.sems.at[slot], self.dev(peer))

        def start(self):
            peers(self.n, self.me, lambda p: self.copy(p, self.me).start())

        def wait_from(self, p):
            self.copy(p, p).wait_recv()

        def wait(self):
            peers(self.n, self.me, self.wait_from)

        def drain(self):
            peers(self.n, self.me, lambda p: self.copy(p, self.me).wait_send())

    def over_z(src, dst, number, sems):
        return Exchange(nz, z, lambda p: {"smp": z_index(p)}, src, dst, number, sems)

    def over_grp(src, dst, number, sems):
        return Exchange(ng, g, lambda p: {"grp": p}, src, dst, number, sems)

    def over_smp(src, dst, number, sems):
        return Exchange(ns, s, lambda p: {"smp": p}, src, dst, number, sems)

    def lane(k, width=LANES):
        return pl.ds(pl.multiple_of(k * width, width), width)

    def block(k, height=32):
        return pl.ds(pl.multiple_of(k * height, height), height)

    w_copy = pltpu.make_async_copy(w_hbm.at[:, lane(z)], wv, local_sem.at[0])
    w_copy.start()

    barrier = pltpu.get_barrier_semaphore()
    peers(ns, s, lambda p: pl.semaphore_signal(barrier, inc=1, device_id={"smp": p}, device_id_type=MESH))
    peers(ng, g, lambda p: pl.semaphore_signal(barrier, inc=1, device_id={"grp": p}, device_id_type=MESH))

    ex_pk = over_z(lambda p: spk, lambda k: pk.at[k], 0, pk_sem)
    ex_fa = over_z(lambda p: fw.at[:, lane(p)], lambda k: fc.at[q_me, block(k)], 1, fa_sem)
    ex_v1 = over_z(lambda p: vbuf.at[p], lambda k: v1.at[k], 2, v1_sem)
    ex_v2 = over_grp(lambda p: s2, lambda k: r2.at[k], 3, v2_sem)
    ex_v3 = over_smp(lambda p: s3, lambda k: r3.at[k], 4, v3_sem)
    ex_x1 = over_smp(lambda p: x1s, lambda k: x1.at[k], 5, x1_sem)
    ex_x2 = over_smp(lambda p: x2s, lambda k: x2.at[k], 6, x2_sem)
    ex_w1 = over_z(lambda p: vbuf.at[nz + p], lambda k: w1.at[k], 7, w1_sem)
    ex_w2 = over_grp(lambda p: s4, lambda k: r4.at[k], 8, w2_sem)
    ex_w3 = over_smp(lambda p: s5, lambda k: r5.at[k], 9, w3_sem)
    ex_gz = over_z(lambda p: gall.at[q_me, block(p)], lambda k: gown.at[:, lane(k)], 10, gz_sem)

    def gather(buf, first, sems):
        to_core = remote(buf.at[q_me], buf.at[q_me], send.at[first], sems.at[0], {"smp": core})
        to_x = remote(buf.at[q_me], buf.at[q_me], send.at[first + 1], sems.at[1], {"smp": across})
        on = remote(buf.at[q_x], buf.at[q_x], send.at[first + 2], sems.at[2], {"smp": core})
        from_core = remote(buf.at[q_core], buf.at[q_core], send.at[first], sems.at[0], {"smp": core})
        from_x = remote(buf.at[q_x], buf.at[q_x], send.at[first + 1], sems.at[1], {"smp": across})
        from_on = remote(buf.at[q_far], buf.at[q_far], send.at[first + 2], sems.at[2], {"smp": core})
        return to_core, to_x, on, from_core, from_x, from_on

    fx = gather(fc, 11, fx_sem)
    ag = gather(gall, 14, ag_sem)

    bit = jnp.left_shift(jnp.int32(1), lax.broadcasted_iota(jnp.int32, (32, tok), 0))

    def unpack(words, j):
        for xq in range(2):
            for cq in range(2):
                for k in range(nz):
                    row = words[pl.ds(2 * nz * xq + 2 * k + cq, 1), :]
                    up = jnp.where(jnp.bitwise_and(jnp.broadcast_to(row, (32, tok)), bit) != 0, F32(1), F32(-1))
                    at = ((2 * xq + cq) * nz + k) * 32
                    sgn[pl.ds(at, 32), lane(j, tok)] = up.astype(BF16)

    def hidden(j):
        pre = jnp.dot(wt[...], sgn[:, lane(j, tok)], preferred_element_type=F32)
        for r in range(tiles):
            part = pre[:, r * LANES : (r + 1) * LANES] + cols[0]
            hid[:, lane(j * tiles + r)] = jnp.tanh(part)

    cols[0] = jnp.broadcast_to(hb[pl.ds(z, 1), :], (LANES, LANES)).T
    cols[1] = jnp.broadcast_to(fb[pl.ds(z, 1), :], (LANES, LANES)).T
    unpack(spk, 0)
    w_copy.wait()
    for q in range(4):
        parts = [wv[pl.ds(32 * (2 * nz * (q // 2) + 2 * k + q % 2), 32), :] for k in range(nz)]
        wt[:, q * 32 * nz : (q + 1) * 32 * nz] = jnp.concatenate(parts, axis=0).astype(F32).T.astype(BF16)

    pl.semaphore_wait(barrier, ns - 1 + ng - 1)
    ex_fa.start()
    ex_pk.start()
    fc[q_me, block(z), :] = fw[:, lane(z)]
    hidden(0)
    ex_fa.wait()
    fx[0].start()
    fx[1].start()

    def shard(j):
        d = (j + 1) // 2
        return lax.rem(z + (2 * (j % 2) - 1) * d + nz, nz)

    def arrive(j, carry):
        k = shard(j)
        ex_pk.wait_from(k)
        unpack(pk.at[k], j)
        hidden(j)
        return carry

    half = (nz + 1) // 2
    lax.fori_loop(1, half, arrive, 0)
    fx[4].wait_recv()
    fx[2].start()
    lax.fori_loop(half, nz, arrive, 0)
    fx[3].wait_recv()
    fx[5].wait_recv()

    def transposed(buf, q):
        hi, lo = split(buf[q].T)
        at = q * 32 * nz
        ft[:LANES, at : at + 32 * nz] = hi
        ft[LANES:, at : at + 32 * nz] = lo

    def values(base, col):
        def step(j, carry):
            k = shard(j)
            res = jnp.dot(ft[...], sgn[:, lane(j, tok)], preferred_element_type=F32)
            for r in range(tiles):
                both = res[:LANES, r * LANES : (r + 1) * LANES] + res[LANES:, r * LANES : (r + 1) * LANES]
                prod = (both + cols[col]) * hid[:, lane(j * tiles + r)]
                vbuf[base + k, pl.ds(r, 1), :] = jnp.sum(prod, axis=0, keepdims=True)
            return carry
        lax.fori_loop(0, nz, step, 0)

    for q in range(4):
        transposed(fc, q)
    values(0, 1)

    ex_v1.start()
    v1[z] = vbuf[z]
    s2[1] = folded(fw[...] * fw[...]) + folded(fb[...] * fb[...]) * F32(1.0 / ns)
    ex_v1.wait()
    s2[0] = functools.reduce(lambda a, b: a + b, [v1[k] for k in range(nz)])
    ex_v2.start()
    r2[g] = s2[...]
    ex_v2.wait()
    s3[...] = functools.reduce(lambda a, b: a + b, [r2[k] for k in range(ng)])
    ex_v3.start()
    r3[s] = s3[...]
    ex_v3.wait()
    sums = functools.reduce(lambda a, b: a + b, [r3[k] for k in range(ns)])
    mean = total(sums[0]) * F32(1.0 / count)
    norm0 = total(sums[1])
    square = jnp.zeros((8, LANES), F32)
    for k in range(ns):
        off = r3[k, 0] - mean
        square += off * off
    curvature = total(square) * F32(1.0 / count) + F32(LAMBDA) * norm0
    alpha0 = norm0 / curvature

    def weigh(j, carry):
        own = r3[z_index(shard(j)), 0] - mean
        bias = carry
        for r in range(tiles):
            prod = hid[:, lane(j * tiles + r)] * own[r : r + 1, :]
            hi, lo = split(prod)
            ch[:LANES, lane(j * tiles + r)] = hi
            ch[LANES:, lane(j * tiles + r)] = lo
            bias = bias + prod
        return bias

    gb[...] = jnp.zeros((LANES, LANES), F32)

    def weigh_step(j, carry):
        gb[...] = weigh(j, gb[...])
        return carry

    lax.fori_loop(0, nz, weigh_step, 0)
    x1s[...] = jnp.broadcast_to(jnp.sum(gb[...].T, axis=0, keepdims=True), (8, LANES))
    ex_x1.start()
    x1[s] = x1s[...]

    height = 32 * nz

    def image(q):
        res = lax.dot_general(sgn[block(q, height), :], ch[...], (((1,), (1,)), ((), ())), preferred_element_type=F32)
        return res[:, :LANES] + res[:, LANES:]

    hop0 = remote(rs_s.at[0], rs_r.at[0], send.at[17], rs_sem.at[0], {"smp": core})
    hop1 = remote(rs_s.at[1], rs_r.at[1], send.at[18], rs_sem.at[1], {"smp": across})
    hop2 = remote(rs_s.at[2], rs_r.at[2], send.at[19], rs_sem.at[2], {"smp": core})
    rs_s[0] = image(q_far)
    hop0.start()
    part = image(q_x)
    hop0.wait_recv()
    rs_s[1] = part + rs_r[0]
    hop1.start()
    rs_s[2] = image(q_core)
    hop2.start()
    acc[...] = image(q_me)
    hop2.wait_recv()
    acc[...] = acc[...] + rs_r[2]
    hop1.wait_recv()
    gall[q_me] = acc[...] + rs_r[1]
    ag[0].start()
    ag[1].start()
    ex_gz.start()
    gown[:, lane(z)] = gall[q_me, block(z), :]

    ex_x1.wait()
    for k in range(nz):
        at = [x1[2 * nz * xq + 2 * k + cq, 0:1, :] for xq in range(2) for cq in range(2)]
        gb[pl.ds(k, 1), :] = (at[0] + at[1]) + (at[2] + at[3])
    if nz < 8:
        gb[nz:8, :] = jnp.zeros((8 - nz, LANES), F32)
    image_b = gb[:8, :]
    cols[2] = jnp.broadcast_to(gb[pl.ds(z, 1), :], (LANES, LANES)).T
    inv = F32(1.0 / count)
    res_b = fb[...] - alpha0 * (image_b * inv + F32(LAMBDA) * fb[...])
    own_f = fc[q_me]
    res_w = own_f - alpha0 * (gall[q_me] * inv + F32(LAMBDA) * own_f)
    x2s[0] = folded(res_w * res_w) + res_b * res_b * F32(1.0 / ns)
    x2s[1] = folded(res_w * own_f) + res_b * fb[...] * F32(1.0 / ns)
    ex_x2.start()
    x2[s] = x2s[...]
    ag[4].wait_recv()
    ag[2].start()
    ag[3].wait_recv()
    ag[5].wait_recv()
    for q in range(4):
        transposed(gall, q)
    values(nz, 2)

    ex_w1.start()
    w1[z] = vbuf[nz + z]
    ex_x2.wait()
    s4[1:3] = functools.reduce(lambda a, b: a + b, [x2[k] for k in range(ns)])
    ex_w1.wait()
    s4[0] = functools.reduce(lambda a, b: a + b, [w1[k] for k in range(nz)])
    ex_w2.start()
    r4[g] = s4[...]
    ex_w2.wait()
    sums = functools.reduce(lambda a, b: a + b, [r4[k] for k in range(ng)])
    norm1 = total(sums[1])
    cross = total(sums[2])
    beta = norm1 / norm0
    scale_f = F32(1.0) - alpha0 * F32(LAMBDA) + beta
    s5[...] = scale_f * (r3[s, 0] - mean) - (alpha0 * inv) * sums[0]
    ex_w3.start()
    r5[s] = s5[...]
    ex_w3.wait()
    mean1 = total(functools.reduce(lambda a, b: a + b, [r5[k] for k in range(ns)])) * inv
    square = jnp.zeros((8, LANES), F32)
    for k in range(ns):
        off = r5[k] - mean1
        square += off * off
    norm_d = norm1 + F32(2.0) * beta * cross + beta * beta * norm0
    curvature = total(square) * inv + F32(LAMBDA) * norm_d
    alpha1 = norm1 / curvature
    factor_f = alpha0 + alpha1 * scale_f
    factor_g = alpha1 * alpha0 * inv
    ex_gz.wait()
    out_w[...] = factor_f * fw[...] - factor_g * gown[...]
    out_b[...] = factor_f * fb[...] - factor_g * image_b

    for ex in (ex_pk, ex_fa, ex_v1, ex_v2, ex_v3, ex_x1, ex_x2, ex_w1, ex_w2, ex_w3, ex_gz):
        ex.drain()
    for move in (*fx[:3], *ag[:3], hop0, hop1, hop2):
        move.wait_send()


def call(ng, nz, count, spk, w, hb, fw, fb):
    ns = 4 * nz
    tok = spk.shape[1]
    words, height = spk.shape[0], 32 * nz
    nv = 32 * words
    tile = (8, LANES)
    dma = pltpu.SemaphoreType.DMA
    vmem = pl.BlockSpec(memory_space=pltpu.VMEM)
    scratch = [
        pltpu.VMEM((nz, words, tok), jnp.int32),
        pltpu.VMEM((nv, LANES), BF16),
        pltpu.VMEM((LANES, nv), BF16),
        pltpu.VMEM((4, height, LANES), F32),
        pltpu.VMEM((2 * LANES, nv), BF16),
        pltpu.VMEM((nv, nz * tok), BF16),
        pltpu.VMEM((LANES, nz * tok), F32),
        pltpu.VMEM((2 * LANES, nz * tok), BF16),
        pltpu.VMEM((height, LANES), F32),
        pltpu.VMEM((2 * nz, *tile), F32),
        pltpu.VMEM((nz, *tile), F32),
        pltpu.VMEM((2, *tile), F32),
        pltpu.VMEM((ng, 2, *tile), F32),
        pltpu.VMEM((2, *tile), F32),
        pltpu.VMEM((ns, 2, *tile), F32),
        pltpu.VMEM(tile, F32),
        pltpu.VMEM((ns, *tile), F32),
        pltpu.VMEM((2, *tile), F32),
        pltpu.VMEM((ns, 2, *tile), F32),
        pltpu.VMEM((nz, *tile), F32),
        pltpu.VMEM((3, *tile), F32),
        pltpu.VMEM((ng, 3, *tile), F32),
        pltpu.VMEM(tile, F32),
        pltpu.VMEM((ns, *tile), F32),
        pltpu.VMEM((LANES, LANES), F32),
        pltpu.VMEM((3, height, LANES), F32),
        pltpu.VMEM((3, height, LANES), F32),
        pltpu.VMEM((4, height, LANES), F32),
        pltpu.VMEM((32, nz * LANES), F32),
        pltpu.VMEM((3, LANES, LANES), F32),
        dma((1,)),
        dma((20,)),
        dma((nz,)),
        dma((nz,)),
        dma((3,)),
        dma((nz,)),
        dma((ng,)),
        dma((ns,)),
        dma((ns,)),
        dma((ns,)),
        dma((nz,)),
        dma((ng,)),
        dma((ns,)),
        dma((3,)),
        dma((3,)),
        dma((nz,)),
    ]
    return pl.pallas_call(
        functools.partial(kernel, ng, nz, count),
        out_shape=(jax.ShapeDtypeStruct(fw.shape, F32), jax.ShapeDtypeStruct(tile, F32)),
        in_specs=[vmem, pl.BlockSpec(memory_space=pl.ANY), vmem, vmem, vmem],
        out_specs=(vmem, vmem),
        scratch_shapes=scratch,
        compiler_params=pltpu.CompilerParams(collective_id=0, has_side_effects=True,
                                             vmem_limit_bytes=60 * 1024 * 1024),
        name="step",
    )(spk, w, hb, fw, fb)


def solution(mesh):
    ng, ns = mesh.shape["grp"], mesh.shape["smp"]
    nz = ns // 4

    def body(spk, w, hb, fw, fb):
        count = spk.shape[1] * ns
        tile = (8, LANES)
        pad = 8 * LANES - hb.shape[0]
        hb, fb = (jnp.pad(v, (0, pad)).reshape(tile) for v in (hb, fb))
        out_w, out_b = call(ng, nz, count, spk, w, hb, fw, fb)
        return out_w, out_b.reshape(-1)[: nz * LANES]

    return jax.shard_map(body, mesh=mesh,
                         in_specs=(P(None, "smp"), P(None, "grp"), P("grp"), P("smp", "grp"), P("grp")),
                         out_specs=(P("smp", "grp"), P("grp")), check_vma=False)
```

```python
import functools

import jax
import jax.numpy as jnp
from jax import lax
from jax.experimental import pallas as pl
from jax.experimental.pallas import tpu as pltpu
from jax.sharding import PartitionSpec as P

MESH = pl.DeviceIdType.MESH
LAMBDA = 0.01
F32 = jnp.float32
BF16 = jnp.bfloat16
LANES = 128


def split(x):
    hi = x.astype(BF16)
    return hi, (x - hi.astype(F32)).astype(BF16)


def folded(x):
    rows, cols = x.shape
    tiles = [x[r : r + 8, k : k + LANES] for r in range(0, rows, 8) for k in range(0, cols, LANES)]
    return functools.reduce(lambda a, b: a + b, tiles)


def total(x):
    return jnp.sum(jnp.sum(x, axis=0, keepdims=True), axis=1, keepdims=True)


def row_of(x):
    return jnp.sum(x, axis=0, keepdims=True)


def added(parts):
    return functools.reduce(lambda a, b: a + b, parts)


def kernel(ng, nz, count, spk_h, w_h, hb_h, fw_h, fb_h, out_w_h, out_b_h,
           spk, fw, hb, fb, out_w, out_b, pk, wv, wt, fc, ft, sgn, hid, ch,
           vbuf, v1, v2, v3, v2s, v3s, w1, w2, w2s,
           p1s, p1, p2s, p2, p3s, p3, n1s, n1, n2s, n2, b1s, b1, b2s, b2, m1s, m1, x2s, x2, x3s, x3, w3s, w3,
           gb, gi, rs_s, rs_r, gall, gown, cols,
           local_sem, send, recv, near_sem, out_sem, on_sem, fx_sem, rs_sem, ag_sem):
    ns = 4 * nz
    tok = spk.shape[1]
    tiles = tok // LANES
    height = 32 * nz
    s = lax.axis_index("smp")
    g = lax.axis_index("grp")
    xh = s // (2 * nz)
    z = (s // 2) % nz
    c = s % 2
    q_me = 2 * xh + c
    q_core = 2 * xh + 1 - c
    q_x = 2 * (1 - xh) + c
    q_far = 2 * (1 - xh) + 1 - c
    core = s + 1 - 2 * c
    across = s + (2 * nz) * (1 - 2 * xh)

    def z_index(k):
        return 2 * nz * xh + 2 * k + c

    def remote(src, dst, ssem, rsem, dev):
        return pltpu.make_async_remote_copy(src_ref=src, dst_ref=dst, send_sem=ssem, recv_sem=rsem,
                                            device_id=dev, device_id_type=MESH)

    def peers(n, me, act, low=1, high=None):
        def step(j, carry):
            act(lax.rem(me + j, n))
            return carry
        lax.fori_loop(low, n if high is None else high, step, 0)

    def all_of(region, number, sent):
        move = remote(region, region, send.at[number], recv.at[number], {"smp": core})
        move.wait_send() if sent else move.wait_recv()

    class Exchange:
        def __init__(self, n, me, dev, src, dst, number, region):
            self.n, self.me, self.dev, self.src, self.dst = n, me, dev, src, dst
            self.number, self.region = number, region

        def start(self):
            peers(self.n, self.me, lambda p: remote(self.src(p), self.dst(self.me), send.at[self.number],
                                                    recv.at[self.number], self.dev(p)).start())

        def wait(self):
            all_of(self.region, self.number, False)

        def drain(self):
            all_of(self.region, self.number, True)

    def rows_of(buf, n, dst):
        return buf.at[pl.ds(0, n - 1)] if dst is None else dst

    def over_z(src, buf, number, dst=None, region=None):
        return Exchange(nz, z, lambda p: {"smp": z_index(p)}, src, dst or (lambda k: buf.at[k]), number,
                        rows_of(buf, nz, region))

    def over_grp(src, buf, number):
        return Exchange(ng, g, lambda p: {"grp": p}, src, lambda k: buf.at[k], number, rows_of(buf, ng, None))

    def quad_index(q):
        return 2 * nz * (q // 2) + 2 * z + q % 2

    def over_quad(src, buf, number):
        return Exchange(4, q_me, lambda p: {"smp": quad_index(p)}, src, lambda k: buf.at[k], number,
                        rows_of(buf, 4, None))

    plane = 4 * g + q_me
    quads = [quad_index(lax.rem(q_me + d, 4)) for d in range(4)]

    def over_all(do):
        for index in quads[1:]:
            do({"grp": g, "smp": index})

        def step(j, carry):
            h = lax.rem(g + j, ng)
            for index in quads:
                do({"grp": h, "smp": index})
            return carry
        lax.fori_loop(1, ng, step, 0)

    class Plane:
        def __init__(self, src, buf, number):
            self.src, self.buf, self.number = src, buf, number
            self.region = buf.at[pl.ds(0, 4 * ng - 1)]

        def start(self):
            over_all(lambda dev: remote(self.src, self.buf.at[plane], send.at[self.number], recv.at[self.number],
                                        dev).start())

        def wait(self):
            all_of(self.region, self.number, False)

        def drain(self):
            all_of(self.region, self.number, True)

    def lane(k, width=LANES):
        return pl.ds(pl.multiple_of(k * width, width), width)

    def block(k, size=32):
        return pl.ds(pl.multiple_of(k * size, size), size)

    loads = [pltpu.make_async_copy(a, b, local_sem.at[i]) for i, (a, b) in enumerate(
        ((spk_h, spk), (w_h.at[:, lane(z)], wv), (hb_h, hb), (fb_h, fb), (fw_h, fw)))]
    for load in loads:
        load.start()
    barrier = pltpu.get_barrier_semaphore()
    peers(nz, z, lambda p: pl.semaphore_signal(barrier, inc=1, device_id={"smp": z_index(p)}, device_id_type=MESH))
    over_all(lambda dev: pl.semaphore_signal(barrier, inc=1, device_id=dev, device_id_type=MESH))

    ex_fa = over_z(lambda p: fw.at[:, lane(p)], fc, 0, lambda k: fc.at[q_me, block(k)],
                   fc.at[q_me, pl.ds(0, 32 * (nz - 1))])
    ex_v1 = over_grp(lambda p: vbuf.at[p], v1, 1)
    ex_v2 = over_z(lambda p: v2s, v2, 2)
    ex_v3 = over_grp(lambda p: v3s, v3, 3)
    ex_w1 = over_grp(lambda p: vbuf.at[nz + p], w1, 4)
    ex_w2 = over_z(lambda p: w2s, w2, 5)
    ex_w3 = Plane(w3s, w3, 6)
    ex_p1 = over_grp(lambda p: p1s, p1, 7)
    ex_p2 = over_z(lambda p: p2s, p2, 8)
    ex_p3 = over_quad(lambda p: p3s, p3, 9)
    ex_n1 = Plane(n1s, n1, 10)
    ex_n2 = over_z(lambda p: n2s, n2, 11)
    ex_b1 = over_quad(lambda p: b1s, b1, 12)
    ex_b2 = over_z(lambda p: b2s, b2, 13)
    ex_m1 = Plane(m1s, m1, 29)
    ex_x2 = Plane(x2s, x2, 14)
    ex_x3 = over_z(lambda p: x3s, x3, 30)
    ex_gz = over_z(lambda p: gall.at[q_me, block(p)], gown, 15, lambda k: gown.at[:, lane(k)],
                   gown.at[:, pl.ds(0, LANES * (nz - 1))])

    def gather(buf, first, sems):
        to_core = remote(buf.at[q_me], buf.at[q_me], send.at[first], sems.at[0], {"smp": core})
        to_x = remote(buf.at[q_me], buf.at[q_me], send.at[first + 1], sems.at[1], {"smp": across})
        on = remote(buf.at[q_x], buf.at[q_x], send.at[first + 2], sems.at[2], {"smp": core})
        from_core = remote(buf.at[q_core], buf.at[q_core], send.at[first], sems.at[0], {"smp": core})
        from_x = remote(buf.at[q_x], buf.at[q_x], send.at[first + 1], sems.at[1], {"smp": across})
        from_on = remote(buf.at[q_far], buf.at[q_far], send.at[first + 2], sems.at[2], {"smp": core})
        return to_core, to_x, on, from_core, from_x, from_on

    fx = gather(fc, 16, fx_sem)
    ag = gather(gall, 19, ag_sem)

    piece = tok // ng
    up, down = lax.rem(z + 1, nz), lax.rem(z + nz - 1, nz)
    near = [remote(spk, pk.at[z], send.at[22 + i], near_sem.at[i], {"smp": z_index(k)})
            for i, k in enumerate((up, down))]
    from_near = [remote(spk, pk.at[k], send.at[22 + i], near_sem.at[i], {"smp": z_index(up)})
                 for i, k in enumerate((down, up))]

    def far_out(k):
        return remote(spk.at[:, lane(g, piece)], pk.at[z, :, lane(g, piece)], send.at[24], out_sem.at[z],
                      {"smp": z_index(k)})

    def far_first(k):
        part = pk.at[k, :, lane(g, piece)]
        return remote(part, part, send.at[24], out_sem.at[k], {"smp": z_index(k)})

    def far_on(k, h):
        part = pk.at[k, :, lane(g, piece)]
        return remote(part, part, send.at[25], on_sem.at[k], {"grp": h})

    def far_rest(k):
        part = pk.at[k, :, pl.ds(0, piece * (ng - 1))]
        return remote(part, part, send.at[25], on_sem.at[k], {"smp": core})

    bit = jnp.left_shift(jnp.int32(1), lax.broadcasted_iota(jnp.int32, (16, tok), 0)).astype(jnp.int16)

    def unpack(words, j):
        for xq in range(2):
            for cq in range(2):
                for k in range(nz):
                    row = words[pl.ds(2 * nz * xq + 2 * k + cq, 1), :]
                    at = ((2 * xq + cq) * nz + k) * 32
                    for half in range(2):
                        word = jnp.right_shift(row, 16 * half) if half else row
                        word = jnp.broadcast_to(word, (16, tok)).astype(jnp.int16)
                        sgn[pl.ds(at + 16 * half, 16), lane(j, tok)] = jnp.where(
                            jnp.bitwise_and(word, bit) != 0, BF16(1), BF16(-1))

    def hidden(j):
        pre = jnp.dot(wt[...], sgn[:, lane(j, tok)], preferred_element_type=F32)
        for r in range(tiles):
            part = pre[:, r * LANES : (r + 1) * LANES] + cols[0]
            hid[:, lane(j * tiles + r)] = jnp.tanh(part)

    loads[0].wait()
    unpack(spk, 0)
    loads[1].wait()
    loads[2].wait()
    loads[3].wait()
    cols[0] = jnp.broadcast_to(hb[pl.ds(z, 1), :], (LANES, LANES)).T
    cols[1] = jnp.broadcast_to(fb[pl.ds(z, 1), :], (LANES, LANES)).T
    for q in range(4):
        parts = [wv[pl.ds(32 * (2 * nz * (q // 2) + 2 * k + q % 2), 32), :] for k in range(nz)]
        wt[:, q * height : (q + 1) * height] = jnp.concatenate(parts, axis=0).astype(F32).T.astype(BF16)
    loads[4].wait()
    n1s[...] = row_of(folded(fw[...] * fw[...]) + folded(fb[...] * fb[...]) * F32(1.0 / ns))

    pl.semaphore_wait(barrier, nz - 1 + 4 * ng - 1)
    ex_fa.start()
    peers(nz, z, lambda k: far_out(k).start(), 2, nz - 1)
    for move in near:
        move.start()
    fc[q_me, block(z), :] = fw[:, lane(z)]
    hidden(0)
    ex_n1.start()
    n1[plane] = n1s[...]
    ex_fa.wait()
    fx[0].start()
    fx[1].start()

    def pass_on(k):
        far_first(k).wait_recv()
        peers(ng, g, lambda h: far_on(k, h).start())

    peers(nz, z, pass_on, 2, nz - 1)

    def shard(j):
        d = (j + 1) // 2
        return lax.rem(z + (2 * (j % 2) - 1) * d + nz, nz)

    def transposed(buf, q):
        hi, lo = split(buf[q].T)
        ft[:LANES, lane(q, height)] = hi
        ft[LANES:, lane(q, height)] = lo

    def values(j, base, col, first, width, more=False):
        k = shard(j)
        span = pl.ds(pl.multiple_of(first, 2 * height), width)
        res = jnp.dot(ft[:, span], sgn[span, lane(j, tok)], preferred_element_type=F32)
        for r in range(tiles):
            both = res[:LANES, r * LANES : (r + 1) * LANES] + res[LANES:, r * LANES : (r + 1) * LANES]
            if col is not None:
                both = both + cols[col]
            got = row_of(both * hid[:, lane(j * tiles + r)])
            at = (base + k, pl.ds(r, 1), slice(None))
            vbuf[at] = vbuf[at] + got if more else got

    def each(low, high, act):
        def step(j, carry):
            act(j)
            return carry
        lax.fori_loop(low, high, step, 0)

    for i in (1, 0):
        from_near[i].wait_recv()
        unpack(pk.at[(down, up)[i]], 2 - i)
        hidden(2 - i)
    fx[4].wait_recv()
    fx[2].start()
    fx[3].wait_recv()
    transposed(fc, q_me)
    transposed(fc, q_core)
    transposed(fc, q_x)
    fx[5].wait_recv()
    transposed(fc, q_far)
    each(0, 3, lambda j: values(j, 0, 1, 0, 4 * height))

    def arrive(j):
        k = shard(j)
        far_rest(k).wait_recv()
        unpack(pk.at[k], j)
        hidden(j)
        values(j, 0, 1, 0, 4 * height)

    each(3, nz, arrive)

    ex_v1.start()
    p1s[...] = row_of(added([vbuf[k] for k in range(nz)]))
    ex_p1.start()
    v1[g] = vbuf[g]
    p1[g] = p1s[...]
    ex_n1.wait()
    n2s[...] = added([n1[k] for k in range(4 * ng)])
    ex_n2.start()
    n2[z] = n2s[...]
    ex_v1.wait()
    v2s[...] = added([v1[k] for k in range(ng)])
    ex_v2.start()
    ex_p1.wait()
    p2s[...] = added([p1[k] for k in range(ng)])
    ex_p2.start()
    v2[z] = v2s[...]
    p2[z] = p2s[...]
    ex_fa.drain()
    ex_v1.drain()
    ex_p1.drain()
    ex_n1.drain()
    for move in near:
        move.wait_send()
    peers(nz, z, lambda k: far_out(k).wait_send(), 2, nz - 1)
    ex_v2.wait()
    v3s[...] = added([v2[k] for k in range(nz)])
    ex_v3.start()
    ex_p2.wait()
    p3s[...] = added([p2[k] for k in range(nz)])
    ex_p3.start()
    v3[g] = v3s[...]
    p3[q_me] = p3s[...]
    ex_v2.drain()
    ex_p2.drain()
    peers(nz, z, lambda k: far_rest(k).wait_send(), 2, nz - 1)
    ex_v3.wait()
    ex_p3.wait()
    inv = F32(1.0 / count)
    mean = total(added([p3[k] for k in range(4)])) * inv
    gb[...] = jnp.zeros((LANES, LANES), F32)

    def weigh(j):
        own = v3[shard(j)] - mean
        bias = gb[...]
        for r in range(tiles):
            prod = hid[:, lane(j * tiles + r)] * own[r : r + 1, :]
            hi, lo = split(prod)
            ch[:LANES, lane(j * tiles + r)] = hi
            ch[LANES:, lane(j * tiles + r)] = lo
            bias = bias + prod
        gb[...] = bias

    each(0, nz, weigh)

    once = (s + ns) // ns

    def image(q, slot):
        def run(_):
            res = lax.dot_general(sgn[block(q, height), :], ch[...], (((1,), (1,)), ((), ())),
                                  preferred_element_type=F32)
            gi[slot] = res[:, :LANES] + res[:, LANES:]
        each(0, once, run)

    hop0 = remote(gi.at[0], rs_r.at[0], send.at[26], rs_sem.at[0], {"smp": core})
    hop1 = remote(rs_s, rs_r.at[1], send.at[27], rs_sem.at[1], {"smp": across})
    hop2 = remote(gi.at[1], rs_r.at[2], send.at[28], rs_sem.at[2], {"smp": core})
    image(q_far, 0)
    hop0.start()
    image(q_x, 2)
    b1s[...] = row_of(gb[...].T)
    off = v3s[...] - mean
    m1s[...] = row_of(off * off)
    ex_b1.start()
    b1[q_me] = b1s[...]
    hop0.wait_recv()
    rs_s[...] = gi[2] + rs_r[0]
    hop1.start()
    image(q_core, 1)
    hop2.start()
    ex_m1.start()
    m1[plane] = m1s[...]
    image(q_me, 3)
    ex_b1.wait()
    b2s[...] = added([b1[k] for k in range(4)])
    ex_b2.start()
    b2[z] = b2s[...]
    cols[2] = jnp.broadcast_to(b2s[...], (LANES, LANES)).T
    ex_v3.drain()
    ex_p3.drain()
    ex_b1.drain()
    ex_n2.wait()
    ex_n2.drain()
    norm0 = total(added([n2[k] for k in range(nz)]))
    hop2.wait_recv()
    gi[3] = gi[3] + rs_r[2]
    hop1.wait_recv()
    gall[q_me] = gi[3] + rs_r[1]
    ag[1].start()
    ag[0].start()
    ex_gz.start()
    gown[:, lane(z)] = gall[q_me, block(z), :]
    transposed(gall, q_me)
    ag[3].wait_recv()
    transposed(gall, q_core)
    each(0, nz, lambda j: values(j, nz, 2, xh * 2 * height, 2 * height))

    ex_b2.wait()
    ex_m1.wait()
    for k in range(nz):
        gb[pl.ds(k, 1), :] = b2[k]
    if nz < 8:
        gb[nz:8, :] = jnp.zeros((8 - nz, LANES), F32)
    image_b = gb[:8, :]
    curvature = total(added([m1[k] for k in range(4 * ng)])) * inv + F32(LAMBDA) * norm0
    alpha0 = norm0 / curvature
    res_b = fb[...] - alpha0 * (image_b * inv + F32(LAMBDA) * fb[...])
    own_f = fc[q_me]
    res_w = own_f - alpha0 * (gall[q_me] * inv + F32(LAMBDA) * own_f)
    x2s[0:1] = row_of(folded(res_w * res_w) + res_b * res_b * F32(1.0 / ns))
    x2s[1:2] = row_of(folded(res_w * own_f) + res_b * fb[...] * F32(1.0 / ns))
    ex_x2.start()
    x2[plane] = x2s[...]
    ag[4].wait_recv()
    ag[2].start()
    transposed(gall, q_x)
    ag[5].wait_recv()
    transposed(gall, q_far)
    each(0, nz, lambda j: values(j, nz, None, (1 - xh) * 2 * height, 2 * height, True))

    ex_w1.start()
    w1[g] = vbuf[nz + g]
    ex_x2.wait()
    x3s[...] = added([x2[k] for k in range(4 * ng)])
    ex_x3.start()
    x3[z] = x3s[...]
    for move in (*fx[:3], *ag[:3], hop0, hop1, hop2):
        move.wait_send()
    for ex in (ex_m1, ex_b2, ex_gz):
        ex.drain()
    ex_gz.wait()
    ex_w1.wait()
    w2s[...] = added([w1[k] for k in range(ng)])
    ex_w2.start()
    w2[z] = w2s[...]
    ex_w1.drain()
    ex_x2.drain()
    ex_x3.wait()
    ex_x3.drain()
    sums = added([x3[k] for k in range(nz)])
    norm1 = total(sums[0:1])
    cross = total(sums[1:2])
    beta = norm1 / norm0
    scale_f = F32(1.0) - alpha0 * F32(LAMBDA) + beta
    norm_d = norm1 + F32(2.0) * beta * cross + beta * beta * norm0
    ex_w2.wait()
    mixed = scale_f * off - (alpha0 * inv) * added([w2[k] for k in range(nz)])
    here = total(mixed)
    spread = mixed - here * F32(1.0 / tok)
    w3s[0:1] = jnp.broadcast_to(here, (1, LANES))
    w3s[1:2] = row_of(spread * spread)
    ex_w3.start()
    w3[plane] = w3s[...]
    ex_w2.drain()
    ex_w3.wait()
    shards = [w3[k, 0:1, :] for k in range(4 * ng)]
    mean1 = added(shards) * inv
    between = row_of(jnp.zeros((1, LANES), F32))
    for one in shards:
        gap = one * F32(1.0 / tok) - mean1
        between += gap * gap
    within = total(added([w3[k, 1:2, :] for k in range(4 * ng)]))
    square = within + between[:, 0:1] * F32(tok)
    curvature = square * inv + F32(LAMBDA) * norm_d
    alpha1 = norm1 / curvature
    factor_f = alpha0 + alpha1 * scale_f
    factor_g = alpha1 * alpha0 * inv
    out_w[...] = factor_f * fw[...] - factor_g * gown[...]
    out_b[...] = factor_f * fb[...] - factor_g * image_b
    stores = [pltpu.make_async_copy(a, b, local_sem.at[5 + i]) for i, (a, b) in enumerate(
        ((out_w, out_w_h), (out_b, out_b_h)))]
    for store in stores:
        store.start()
    ex_w3.drain()
    for store in stores:
        store.wait()


def call(ng, nz, count, spk, w, hb, fw, fb):
    ns = 4 * nz
    tok = spk.shape[1]
    words, height = spk.shape[0], 32 * nz
    nv = 32 * words
    tile = (8, LANES)
    dma = pltpu.SemaphoreType.DMA
    anywhere = pl.BlockSpec(memory_space=pl.ANY)

    def f32(*shape):
        return pltpu.VMEM(shape, F32)

    scratch = [
        pltpu.VMEM((words, tok), jnp.int32), f32(*fw.shape), f32(*tile), f32(*tile), f32(*fw.shape), f32(*tile),
        pltpu.VMEM((nz, words, tok), jnp.int32),
        pltpu.VMEM((nv, LANES), BF16),
        pltpu.VMEM((LANES, nv), BF16),
        f32(4, height, LANES),
        pltpu.VMEM((2 * LANES, nv), BF16),
        pltpu.VMEM((nv, nz * tok), BF16),
        f32(LANES, nz * tok),
        pltpu.VMEM((2 * LANES, nz * tok), BF16),
        f32(2 * nz, *tile), f32(ng, *tile), f32(nz, *tile), f32(ng, *tile), f32(*tile), f32(*tile),
        f32(ng, *tile), f32(nz, *tile), f32(*tile),
        f32(1, LANES), f32(ng, 1, LANES), f32(1, LANES), f32(nz, 1, LANES), f32(1, LANES), f32(4, 1, LANES),
        f32(1, LANES), f32(4 * ng, 1, LANES), f32(1, LANES), f32(nz, 1, LANES),
        f32(1, LANES), f32(4, 1, LANES), f32(1, LANES), f32(nz, 1, LANES), f32(1, LANES), f32(4 * ng, 1, LANES),
        f32(2, LANES), f32(4 * ng, 2, LANES), f32(2, LANES), f32(nz, 2, LANES), f32(2, LANES), f32(4 * ng, 2, LANES),
        f32(LANES, LANES), f32(4, height, LANES), f32(height, LANES), f32(3, height, LANES), f32(4, height, LANES),
        f32(32, nz * LANES), f32(3, LANES, LANES),
        dma((7,)), dma((31,)), dma((31,)), dma((2,)), dma((nz,)), dma((nz,)), dma((3,)), dma((3,)), dma((3,)),
    ]
    return pl.pallas_call(
        functools.partial(kernel, ng, nz, count),
        out_shape=(jax.ShapeDtypeStruct(fw.shape, F32), jax.ShapeDtypeStruct(tile, F32)),
        in_specs=[anywhere] * 5,
        out_specs=(anywhere, anywhere),
        scratch_shapes=scratch,
        compiler_params=pltpu.CompilerParams(collective_id=0, has_side_effects=True,
                                             vmem_limit_bytes=60 * 1024 * 1024),
        name="step",
    )(spk, w, hb, fw, fb)


def solution(mesh):
    ng, ns = mesh.shape["grp"], mesh.shape["smp"]
    nz = ns // 4

    def body(spk, w, hb, fw, fb):
        count = spk.shape[1] * ns
        tile = (8, LANES)
        pad = 8 * LANES - hb.shape[0]
        hb, fb = (jnp.pad(v, (0, pad)).reshape(tile) for v in (hb, fb))
        out_w, out_b = call(ng, nz, count, spk, w, hb, fw, fb)
        return out_w, out_b.reshape(-1)[: nz * LANES]

    return jax.shard_map(body, mesh=mesh,
                         in_specs=(P(None, "smp"), P(None, "grp"), P("grp"), P("smp", "grp"), P("grp")),
                         out_specs=(P("smp", "grp"), P("grp")), check_vma=False)
```

```python
import functools

import jax
import jax.numpy as jnp
from jax import lax
from jax.experimental import pallas as pl
from jax.experimental.pallas import tpu as pltpu
from jax.sharding import PartitionSpec as P

MESH = pl.DeviceIdType.MESH
LAMBDA = 0.01
F32 = jnp.float32
BF16 = jnp.bfloat16
LANES = 128


def split(x):
    hi = x.astype(BF16)
    return hi, (x - hi.astype(F32)).astype(BF16)


def folded(x):
    rows, cols = x.shape
    tiles = [x[r : r + 8, k : k + LANES] for r in range(0, rows, 8) for k in range(0, cols, LANES)]
    return functools.reduce(lambda a, b: a + b, tiles)


def total(x):
    return jnp.sum(jnp.sum(x, axis=0, keepdims=True), axis=1, keepdims=True)


def row_of(x):
    return jnp.sum(x, axis=0, keepdims=True)


def added(parts):
    return functools.reduce(lambda a, b: a + b, parts)


def kernel(ng, nz, count, spk_h, w_h, hb_h, fw_h, fb_h, out_w_h, out_b_h,
           spk, fw, hb, fb, out_w, out_b, pk, wv, wt, fc, ft, sgn, hid, ch,
           vbuf, v1, v2, v3, v2s, v3s, w1, w2, w2s,
           p1s, p1, p2s, p2, p3s, p3, n1s, n1, n2s, n2, b1s, b1, b2s, b2, m1s, m1, x2s, x2, x3s, x3, w3s, w3,
           gb, gi, rs_s, rs_r, gall, gown, cols,
           local_sem, send, recv, near_sem, fa_sem, out_sem, on_sem, fx_sem, rs_sem, ag_sem):
    ns = 4 * nz
    tok = spk.shape[1]
    tiles = tok // LANES
    height = 32 * nz
    s = lax.axis_index("smp")
    g = lax.axis_index("grp")
    xh = s // (2 * nz)
    z = (s // 2) % nz
    c = s % 2
    q_me = 2 * xh + c
    q_core = 2 * xh + 1 - c
    q_x = 2 * (1 - xh) + c
    q_far = 2 * (1 - xh) + 1 - c
    core = s + 1 - 2 * c
    across = s + (2 * nz) * (1 - 2 * xh)

    def z_index(k):
        return 2 * nz * xh + 2 * k + c

    def remote(src, dst, ssem, rsem, dev):
        return pltpu.make_async_remote_copy(src_ref=src, dst_ref=dst, send_sem=ssem, recv_sem=rsem,
                                            device_id=dev, device_id_type=MESH)

    def peers(n, me, act, low=1, high=None):
        def step(j, carry):
            act(lax.rem(me + j, n))
            return carry
        lax.fori_loop(low, n if high is None else high, step, 0)

    def all_of(region, number, sent):
        move = remote(region, region, send.at[number], recv.at[number], {"smp": core})
        move.wait_send() if sent else move.wait_recv()

    class Exchange:
        def __init__(self, n, me, dev, src, dst, number, region):
            self.n, self.me, self.dev, self.src, self.dst = n, me, dev, src, dst
            self.number, self.region = number, region

        def start(self):
            peers(self.n, self.me, lambda p: remote(self.src(p), self.dst(self.me), send.at[self.number],
                                                    recv.at[self.number], self.dev(p)).start())

        def wait(self):
            all_of(self.region, self.number, False)

        def drain(self):
            all_of(self.region, self.number, True)

    def rows_of(buf, n, dst):
        return buf.at[pl.ds(0, n - 1)] if dst is None else dst

    def over_z(src, buf, number, dst=None, region=None):
        return Exchange(nz, z, lambda p: {"smp": z_index(p)}, src, dst or (lambda k: buf.at[k]), number,
                        rows_of(buf, nz, region))

    def over_grp(src, buf, number):
        return Exchange(ng, g, lambda p: {"grp": p}, src, lambda k: buf.at[k], number, rows_of(buf, ng, None))

    def quad_index(q):
        return 2 * nz * (q // 2) + 2 * z + q % 2

    def over_quad(src, buf, number):
        return Exchange(4, q_me, lambda p: {"smp": quad_index(p)}, src, lambda k: buf.at[k], number,
                        rows_of(buf, 4, None))

    plane = 4 * g + q_me
    quads = [quad_index(lax.rem(q_me + d, 4)) for d in range(4)]

    def over_all(do):
        for index in quads[1:]:
            do({"grp": g, "smp": index})

        def step(j, carry):
            h = lax.rem(g + j, ng)
            for index in quads:
                do({"grp": h, "smp": index})
            return carry
        lax.fori_loop(1, ng, step, 0)

    class Plane:
        def __init__(self, src, buf, number):
            self.src, self.buf, self.number = src, buf, number
            self.region = buf.at[pl.ds(0, 4 * ng - 1)]

        def start(self):
            over_all(lambda dev: remote(self.src, self.buf.at[plane], send.at[self.number], recv.at[self.number],
                                        dev).start())

        def wait(self):
            all_of(self.region, self.number, False)

        def drain(self):
            all_of(self.region, self.number, True)

    def lane(k, width=LANES):
        return pl.ds(pl.multiple_of(k * width, width), width)

    def block(k, size=32):
        return pl.ds(pl.multiple_of(k * size, size), size)

    loads = [pltpu.make_async_copy(a, b, local_sem.at[i]) for i, (a, b) in enumerate(
        ((spk_h, spk), (w_h.at[:, lane(z)], wv), (hb_h, hb), (fb_h, fb), (fw_h, fw)))]
    for load in loads:
        load.start()
    barrier = pltpu.get_barrier_semaphore()
    peers(nz, z, lambda p: pl.semaphore_signal(barrier, inc=1, device_id={"smp": z_index(p)}, device_id_type=MESH))
    over_all(lambda dev: pl.semaphore_signal(barrier, inc=1, device_id=dev, device_id_type=MESH))

    ex_v1 = over_grp(lambda p: vbuf.at[p], v1, 1)
    ex_v2 = over_z(lambda p: v2s, v2, 2)
    ex_v3 = over_grp(lambda p: v3s, v3, 3)
    ex_w1 = over_grp(lambda p: vbuf.at[nz + p], w1, 4)
    ex_w2 = over_z(lambda p: w2s, w2, 5)
    ex_w3 = Plane(w3s, w3, 6)
    ex_p1 = over_grp(lambda p: p1s, p1, 7)
    ex_p2 = over_z(lambda p: p2s, p2, 8)
    ex_p3 = over_quad(lambda p: p3s, p3, 9)
    ex_n1 = Plane(n1s, n1, 10)
    ex_n2 = over_z(lambda p: n2s, n2, 11)
    ex_b1 = over_quad(lambda p: b1s, b1, 12)
    ex_b2 = over_z(lambda p: b2s, b2, 13)
    ex_m1 = Plane(m1s, m1, 29)
    ex_x2 = Plane(x2s, x2, 14)
    ex_x3 = over_z(lambda p: x3s, x3, 30)
    ex_gz = over_z(lambda p: gall.at[q_me, block(p)], gown, 15, lambda k: gown.at[:, lane(k)],
                   gown.at[:, pl.ds(0, LANES * (nz - 1))])

    def gather(buf, first, sems):
        to_core = remote(buf.at[q_me], buf.at[q_me], send.at[first], sems.at[0], {"smp": core})
        to_x = remote(buf.at[q_me], buf.at[q_me], send.at[first + 1], sems.at[1], {"smp": across})
        on = remote(buf.at[q_x], buf.at[q_x], send.at[first + 2], sems.at[2], {"smp": core})
        from_core = remote(buf.at[q_core], buf.at[q_core], send.at[first], sems.at[0], {"smp": core})
        from_x = remote(buf.at[q_x], buf.at[q_x], send.at[first + 1], sems.at[1], {"smp": across})
        from_on = remote(buf.at[q_far], buf.at[q_far], send.at[first + 2], sems.at[2], {"smp": core})
        return to_core, to_x, on, from_core, from_x, from_on

    fx = gather(fc, 16, fx_sem)

    piece = tok // ng
    up, down = lax.rem(z + 1, nz), lax.rem(z + nz - 1, nz)
    near = [remote(spk, pk.at[z], send.at[22 + i], near_sem.at[i], {"smp": z_index(k)})
            for i, k in enumerate((up, down))]
    from_near = [remote(spk, pk.at[k], send.at[22 + i], near_sem.at[i], {"smp": z_index(up)})
                 for i, k in enumerate((down, up))]

    def force_out(k):
        return remote(fw.at[:, lane(k)], fc.at[q_me, block(z)], send.at[0], fa_sem.at[z], {"smp": z_index(k)})

    def force_in(k):
        part = fc.at[q_me, block(k)]
        return remote(part, part, send.at[0], fa_sem.at[k], {"smp": z_index(k)})

    def force_on(k):
        part = fc.at[q_me, block(k)]
        remote(part, part, send.at[17], fx_sem.at[1], {"smp": across}).start()
        remote(part, part, send.at[16], fx_sem.at[0], {"smp": core}).start()

    def far_out(k):
        return remote(spk.at[:, lane(g, piece)], pk.at[z, :, lane(g, piece)], send.at[24], out_sem.at[z],
                      {"smp": z_index(k)})

    def far_first(k):
        part = pk.at[k, :, lane(g, piece)]
        return remote(part, part, send.at[24], out_sem.at[k], {"smp": z_index(k)})

    def far_on(k, h):
        part = pk.at[k, :, lane(g, piece)]
        return remote(part, part, send.at[25], on_sem.at[k], {"grp": h})

    def far_rest(k):
        part = pk.at[k, :, pl.ds(0, piece * (ng - 1))]
        return remote(part, part, send.at[25], on_sem.at[k], {"smp": core})

    bit = jnp.left_shift(jnp.int32(1), lax.broadcasted_iota(jnp.int32, (16, tok), 0)).astype(jnp.int16)

    def unpack(words, j):
        for xq in range(2):
            for cq in range(2):
                for k in range(nz):
                    row = words[pl.ds(2 * nz * xq + 2 * k + cq, 1), :]
                    at = ((2 * xq + cq) * nz + k) * 32
                    for half in range(2):
                        word = jnp.right_shift(row, 16 * half) if half else row
                        word = jnp.broadcast_to(word, (16, tok)).astype(jnp.int16)
                        sgn[pl.ds(at + 16 * half, 16), lane(j, tok)] = jnp.where(
                            jnp.bitwise_and(word, bit) != 0, BF16(1), BF16(-1))

    def hidden(j):
        pre = jnp.dot(wt[...], sgn[:, lane(j, tok)], preferred_element_type=F32)
        for r in range(tiles):
            part = pre[:, r * LANES : (r + 1) * LANES] + cols[0]
            hid[:, lane(j * tiles + r)] = jnp.tanh(part)

    loads[0].wait()
    unpack(spk, 0)
    loads[1].wait()
    loads[2].wait()
    loads[3].wait()
    cols[0] = jnp.broadcast_to(hb[pl.ds(z, 1), :], (LANES, LANES)).T
    cols[1] = jnp.broadcast_to(fb[pl.ds(z, 1), :], (LANES, LANES)).T
    for q in range(4):
        parts = [wv[pl.ds(32 * (2 * nz * (q // 2) + 2 * k + q % 2), 32), :] for k in range(nz)]
        wt[:, q * height : (q + 1) * height] = jnp.concatenate(parts, axis=0).astype(F32).T.astype(BF16)
    loads[4].wait()
    n1s[...] = row_of(folded(fw[...] * fw[...]) + folded(fb[...] * fb[...]) * F32(1.0 / ns))

    pl.semaphore_wait(barrier, nz - 1 + 4 * ng - 1)
    peers(nz, z, lambda k: force_out(k).start())
    peers(nz, z, lambda k: far_out(k).start(), 2, nz - 1)
    for move in near:
        move.start()
    fc[q_me, block(z), :] = fw[:, lane(z)]
    hidden(0)
    ex_n1.start()
    n1[plane] = n1s[...]
    def shard(j):
        d = (j + 1) // 2
        return lax.rem(z + (2 * (j % 2) - 1) * d + nz, nz)

    def each(low, high, act):
        def step(j, carry):
            act(j)
            return carry
        lax.fori_loop(low, high, step, 0)

    force_on(z)

    def force_pass(j):
        force_in(shard(j)).wait_recv()
        force_on(shard(j))

    each(1, nz, force_pass)

    def pass_on(j):
        k = shard(j)
        far_first(k).wait_recv()
        peers(ng, g, lambda h: far_on(k, h).start())

    each(3, nz, pass_on)

    def transposed(buf, q):
        hi, lo = split(buf[q].T)
        ft[:LANES, lane(q, height)] = hi
        ft[LANES:, lane(q, height)] = lo

    def values(wide, i, base, col, rows, more=False):
        res = jnp.dot(ft[:, rows], sgn[rows, lane(i, wide * tok)], preferred_element_type=F32)
        for n in range(wide):
            k = shard(i * wide + n)
            for r in range(tiles):
                at = (n * tiles + r) * LANES
                both = res[:LANES, at : at + LANES] + res[LANES:, at : at + LANES]
                if col is not None:
                    both = both + cols[col]
                got = row_of(both * hid[:, lane((i * wide + n) * tiles + r)])
                to = (base + k, pl.ds(r, 1), slice(None))
                vbuf[to] = vbuf[to] + got if more else got

    for i in (1, 0):
        from_near[i].wait_recv()
        unpack(pk.at[(down, up)[i]], 2 - i)
        hidden(2 - i)
    def arrive(j):
        k = shard(j)
        far_rest(k).wait_recv()
        unpack(pk.at[k], j)
        hidden(j)

    fx[4].wait_recv()
    fx[2].start()
    fx[3].wait_recv()
    transposed(fc, q_me)
    transposed(fc, q_core)
    transposed(fc, q_x)
    early = min(nz, 5)
    each(3, early, arrive)
    fx[5].wait_recv()
    transposed(fc, q_far)
    every = pl.ds(0, 4 * height)
    wide = nz // 2
    values(wide, 0, 0, 1, every)
    each(early, nz, arrive)
    values(wide, 1, 0, 1, every)

    ex_v1.start()
    p1s[...] = row_of(added([vbuf[k] for k in range(nz)]))
    ex_p1.start()
    v1[g] = vbuf[g]
    p1[g] = p1s[...]
    ex_n1.wait()
    n2s[...] = added([n1[k] for k in range(4 * ng)])
    ex_n2.start()
    n2[z] = n2s[...]
    ex_v1.wait()
    v2s[...] = added([v1[k] for k in range(ng)])
    ex_v2.start()
    ex_p1.wait()
    p2s[...] = added([p1[k] for k in range(ng)])
    ex_p2.start()
    v2[z] = v2s[...]
    p2[z] = p2s[...]
    peers(nz, z, lambda k: force_out(k).wait_send())
    ex_v1.drain()
    ex_p1.drain()
    ex_n1.drain()
    for move in near:
        move.wait_send()
    peers(nz, z, lambda k: far_out(k).wait_send(), 2, nz - 1)
    ex_v2.wait()
    v3s[...] = added([v2[k] for k in range(nz)])
    ex_v3.start()
    ex_p2.wait()
    p3s[...] = added([p2[k] for k in range(nz)])
    ex_p3.start()
    v3[g] = v3s[...]
    p3[q_me] = p3s[...]
    ex_v2.drain()
    ex_p2.drain()
    peers(nz, z, lambda k: far_rest(k).wait_send(), 2, nz - 1)
    ex_v3.wait()
    ex_p3.wait()
    inv = F32(1.0 / count)
    mean = total(added([p3[k] for k in range(4)])) * inv
    once = (s + ns) // ns

    def first_rows(_):
        bias = jnp.zeros((LANES, LANES), F32)
        sums = [None, None]
        for j in range(nz):
            own = v3[shard(j)] - mean
            for r in range(tiles):
                at = (j * tiles + r) * LANES
                prod = hid[:, at : at + LANES] * own[r : r + 1, :]
                hi, lo = split(prod)
                ch[:LANES, at : at + LANES] = hi
                ch[LANES:, at : at + LANES] = lo
                bias = bias + prod
            span = slice(j * tok, (j + 1) * tok)
            for h in range(2):
                res = lax.dot_general(sgn[h * height : (h + 1) * height, span], ch[:, span],
                                      (((1,), (1,)), ((), ())), preferred_element_type=F32)
                sums[h] = res if sums[h] is None else sums[h] + res
        for h in range(2):
            gi[h] = sums[h][:, :LANES] + sums[h][:, LANES:]
        gb[...] = bias

    each(0, once, first_rows)

    def image(q):
        def run(_):
            res = lax.dot_general(sgn[block(q, height), :], ch[...], (((1,), (1,)), ((), ())),
                                  preferred_element_type=F32)
            gi[q] = res[:, :LANES] + res[:, LANES:]
        each(0, once, run)

    mine = (c, 2 + c)
    other = (1 - c, 3 - c)
    to_core = [remote(gi.at[other[i]], rs_r.at[i], send.at[26 + i], rs_sem.at[i], {"smp": core}) for i in range(2)]
    to_x = [remote(rs_s.at[i], rs_r.at[2 + i], send.at[19 + i], rs_sem.at[2 + i], {"smp": across}) for i in range(2)]
    share = [remote(gall.at[mine[i]], gall.at[mine[i]], send.at[21 + 7 * i], ag_sem.at[i], {"smp": core})
             for i in range(2)]
    shared = [remote(gall.at[other[i]], gall.at[other[i]], send.at[21 + 7 * i], ag_sem.at[i], {"smp": core})
              for i in range(2)]
    to_core[0].start()
    image(other[1])
    to_core[1].start()
    b1s[...] = row_of(gb[...].T)
    off = v3s[...] - mean
    m1s[...] = row_of(off * off)
    ex_b1.start()
    b1[q_me] = b1s[...]
    to_core[0].wait_recv()
    rs_s[0] = gi[mine[0]] + rs_r[0]
    to_x[0].start()
    image(mine[1])
    to_core[1].wait_recv()
    rs_s[1] = gi[mine[1]] + rs_r[1]
    to_x[1].start()
    ex_m1.start()
    m1[plane] = m1s[...]
    ex_v3.drain()
    ex_p3.drain()
    ex_n2.wait()
    ex_n2.drain()
    norm0 = total(added([n2[k] for k in range(nz)]))
    ex_b1.wait()
    b2s[...] = added([b1[k] for k in range(4)])
    ex_b2.start()
    b2[z] = b2s[...]
    cols[2] = jnp.broadcast_to(b2s[...], (LANES, LANES)).T
    ex_b1.drain()

    def quarter(q, first=False):
        transposed(gall, q)
        each(0, 2, lambda i: values(wide, i, nz, 2 if first else None, block(q, height), not first))

    to_x[0].wait_recv()
    gall[mine[0]] = rs_s[0] + rs_r[2]
    share[0].start()
    quarter(mine[0], True)
    shared[0].wait_recv()
    quarter(other[0])
    to_x[1].wait_recv()
    gall[mine[1]] = rs_s[1] + rs_r[3]
    share[1].start()
    ex_gz.start()
    gown[:, lane(z)] = gall[q_me, block(z), :]

    ex_b2.wait()
    ex_m1.wait()
    for k in range(nz):
        gb[pl.ds(k, 1), :] = b2[k]
    if nz < 8:
        gb[nz:8, :] = jnp.zeros((8 - nz, LANES), F32)
    image_b = gb[:8, :]
    curvature = total(added([m1[k] for k in range(4 * ng)])) * inv + F32(LAMBDA) * norm0
    alpha0 = norm0 / curvature
    res_b = fb[...] - alpha0 * (image_b * inv + F32(LAMBDA) * fb[...])
    own_f = fc[q_me]
    res_w = own_f - alpha0 * (gall[q_me] * inv + F32(LAMBDA) * own_f)
    x2s[0:1] = row_of(folded(res_w * res_w) + res_b * res_b * F32(1.0 / ns))
    x2s[1:2] = row_of(folded(res_w * own_f) + res_b * fb[...] * F32(1.0 / ns))
    ex_x2.start()
    x2[plane] = x2s[...]
    quarter(mine[1])
    shared[1].wait_recv()
    quarter(other[1])

    ex_w1.start()
    w1[g] = vbuf[nz + g]
    ex_x2.wait()
    x3s[...] = added([x2[k] for k in range(4 * ng)])
    ex_x3.start()
    x3[z] = x3s[...]
    for move in (*fx[:3], *to_core, *to_x, *share):
        move.wait_send()
    for ex in (ex_m1, ex_b2, ex_gz):
        ex.drain()
    ex_gz.wait()
    ex_w1.wait()
    w2s[...] = added([w1[k] for k in range(ng)])
    ex_w2.start()
    w2[z] = w2s[...]
    ex_w1.drain()
    ex_x2.drain()
    ex_x3.wait()
    ex_x3.drain()
    sums = added([x3[k] for k in range(nz)])
    norm1 = total(sums[0:1])
    cross = total(sums[1:2])
    beta = norm1 / norm0
    scale_f = F32(1.0) - alpha0 * F32(LAMBDA) + beta
    norm_d = norm1 + F32(2.0) * beta * cross + beta * beta * norm0
    ex_w2.wait()
    mixed = scale_f * off - (alpha0 * inv) * added([w2[k] for k in range(nz)])
    here = total(mixed)
    spread = mixed - here * F32(1.0 / tok)
    w3s[0:1] = jnp.broadcast_to(here, (1, LANES))
    w3s[1:2] = row_of(spread * spread)
    ex_w3.start()
    w3[plane] = w3s[...]
    ex_w2.drain()
    ex_w3.wait()
    shards = [w3[k, 0:1, :] for k in range(4 * ng)]
    mean1 = added(shards) * inv
    between = row_of(jnp.zeros((1, LANES), F32))
    for one in shards:
        gap = one * F32(1.0 / tok) - mean1
        between += gap * gap
    within = total(added([w3[k, 1:2, :] for k in range(4 * ng)]))
    square = within + between[:, 0:1] * F32(tok)
    curvature = square * inv + F32(LAMBDA) * norm_d
    alpha1 = norm1 / curvature
    factor_f = alpha0 + alpha1 * scale_f
    factor_g = alpha1 * alpha0 * inv
    out_w[...] = factor_f * fw[...] - factor_g * gown[...]
    out_b[...] = factor_f * fb[...] - factor_g * image_b
    stores = [pltpu.make_async_copy(a, b, local_sem.at[5 + i]) for i, (a, b) in enumerate(
        ((out_w, out_w_h), (out_b, out_b_h)))]
    for store in stores:
        store.start()
    ex_w3.drain()
    for store in stores:
        store.wait()


def call(ng, nz, count, spk, w, hb, fw, fb):
    ns = 4 * nz
    tok = spk.shape[1]
    words, height = spk.shape[0], 32 * nz
    nv = 32 * words
    tile = (8, LANES)
    dma = pltpu.SemaphoreType.DMA
    anywhere = pl.BlockSpec(memory_space=pl.ANY)

    def f32(*shape):
        return pltpu.VMEM(shape, F32)

    scratch = [
        pltpu.VMEM((words, tok), jnp.int32), f32(*fw.shape), f32(*tile), f32(*tile), f32(*fw.shape), f32(*tile),
        pltpu.VMEM((nz, words, tok), jnp.int32),
        pltpu.VMEM((nv, LANES), BF16),
        pltpu.VMEM((LANES, nv), BF16),
        f32(4, height, LANES),
        pltpu.VMEM((2 * LANES, nv), BF16),
        pltpu.VMEM((nv, nz * tok), BF16),
        f32(LANES, nz * tok),
        pltpu.VMEM((2 * LANES, nz * tok), BF16),
        f32(2 * nz, *tile), f32(ng, *tile), f32(nz, *tile), f32(ng, *tile), f32(*tile), f32(*tile),
        f32(ng, *tile), f32(nz, *tile), f32(*tile),
        f32(1, LANES), f32(ng, 1, LANES), f32(1, LANES), f32(nz, 1, LANES), f32(1, LANES), f32(4, 1, LANES),
        f32(1, LANES), f32(4 * ng, 1, LANES), f32(1, LANES), f32(nz, 1, LANES),
        f32(1, LANES), f32(4, 1, LANES), f32(1, LANES), f32(nz, 1, LANES), f32(1, LANES), f32(4 * ng, 1, LANES),
        f32(2, LANES), f32(4 * ng, 2, LANES), f32(2, LANES), f32(nz, 2, LANES), f32(2, LANES), f32(4 * ng, 2, LANES),
        f32(LANES, LANES), f32(4, height, LANES), f32(2, height, LANES), f32(4, height, LANES), f32(4, height, LANES),
        f32(32, nz * LANES), f32(3, LANES, LANES),
        dma((7,)), dma((31,)), dma((31,)), dma((2,)), dma((nz,)), dma((nz,)), dma((nz,)), dma((3,)), dma((4,)), dma((2,)),
    ]
    return pl.pallas_call(
        functools.partial(kernel, ng, nz, count),
        out_shape=(jax.ShapeDtypeStruct(fw.shape, F32), jax.ShapeDtypeStruct(tile, F32)),
        in_specs=[anywhere] * 5,
        out_specs=(anywhere, anywhere),
        scratch_shapes=scratch,
        compiler_params=pltpu.CompilerParams(collective_id=0, has_side_effects=True,
                                             vmem_limit_bytes=60 * 1024 * 1024),
        name="step",
    )(spk, w, hb, fw, fb)


def solution(mesh):
    ng, ns = mesh.shape["grp"], mesh.shape["smp"]
    nz = ns // 4

    def body(spk, w, hb, fw, fb):
        count = spk.shape[1] * ns
        tile = (8, LANES)
        pad = 8 * LANES - hb.shape[0]
        hb, fb = (jnp.pad(v, (0, pad)).reshape(tile) for v in (hb, fb))
        out_w, out_b = call(ng, nz, count, spk, w, hb, fw, fb)
        return out_w, out_b.reshape(-1)[: nz * LANES]

    return jax.shard_map(body, mesh=mesh,
                         in_specs=(P(None, "smp"), P(None, "grp"), P("grp"), P("smp", "grp"), P("grp")),
                         out_specs=(P("smp", "grp"), P("grp")), check_vma=False)
```

```python
import functools

import jax
import jax.numpy as jnp
from jax import lax
from jax.experimental import pallas as pl
from jax.experimental.pallas import tpu as pltpu
from jax.sharding import PartitionSpec as P

MESH = pl.DeviceIdType.MESH
LAMBDA = 0.01
F32 = jnp.float32
BF16 = jnp.bfloat16
LANES = 128


def split(x):
    hi = x.astype(BF16)
    return hi, (x - hi.astype(F32)).astype(BF16)


def folded(x):
    rows, cols = x.shape
    tiles = [x[r : r + 8, k : k + LANES] for r in range(0, rows, 8) for k in range(0, cols, LANES)]
    return functools.reduce(lambda a, b: a + b, tiles)


def total(x):
    return jnp.sum(jnp.sum(x, axis=0, keepdims=True), axis=1, keepdims=True)


def row_of(x):
    return jnp.sum(x, axis=0, keepdims=True)


def added(parts):
    return functools.reduce(lambda a, b: a + b, parts)


def kernel(ng, nz, count, spk_h, w_h, hb_h, fw_h, fb_h, out_w_h, out_b_h,
           spk, fw, hb, fb, out_w, out_b, pk, wv, wt, fc, ft, sgn, hid, ch,
           vbuf, v1, v2, v3, v2s, v3s, w1, w2, w2s,
           p1s, p1, p2s, p2, p3s, p3, n1s, n1, n2s, n2, b1s, b1, b2s, b2, m1s, m1, x2s, x2, x3s, x3, w3s, w3,
           gb, gi, rs_s, rs_r, gall, gown, cols,
           local_sem, send, recv, near_sem, fa_sem, out_sem, on_sem, fx_sem, rs_sem, ag_sem):
    ns = 4 * nz
    tok = spk.shape[1]
    tiles = tok // LANES
    height = 32 * nz
    s = lax.axis_index("smp")
    g = lax.axis_index("grp")
    xh = s // (2 * nz)
    z = (s // 2) % nz
    c = s % 2
    q_me = 2 * xh + c
    q_core = 2 * xh + 1 - c
    q_x = 2 * (1 - xh) + c
    q_far = 2 * (1 - xh) + 1 - c
    core = s + 1 - 2 * c
    across = s + (2 * nz) * (1 - 2 * xh)

    def z_index(k):
        return 2 * nz * xh + 2 * k + c

    def remote(src, dst, ssem, rsem, dev):
        return pltpu.make_async_remote_copy(src_ref=src, dst_ref=dst, send_sem=ssem, recv_sem=rsem,
                                            device_id=dev, device_id_type=MESH)

    def peers(n, me, act, low=1, high=None):
        def step(j, carry):
            act(lax.rem(me + j, n))
            return carry
        lax.fori_loop(low, n if high is None else high, step, 0)

    def all_of(region, number, sent):
        move = remote(region, region, send.at[number], recv.at[number], {"smp": core})
        move.wait_send() if sent else move.wait_recv()

    class Exchange:
        def __init__(self, n, me, dev, src, dst, number, region):
            self.n, self.me, self.dev, self.src, self.dst = n, me, dev, src, dst
            self.number, self.region = number, region

        def start(self):
            peers(self.n, self.me, lambda p: remote(self.src(p), self.dst(self.me), send.at[self.number],
                                                    recv.at[self.number], self.dev(p)).start())

        def wait(self):
            all_of(self.region, self.number, False)

        def drain(self):
            all_of(self.region, self.number, True)

    def rows_of(buf, n, dst):
        return buf.at[pl.ds(0, n - 1)] if dst is None else dst

    def over_z(src, buf, number, dst=None, region=None):
        return Exchange(nz, z, lambda p: {"smp": z_index(p)}, src, dst or (lambda k: buf.at[k]), number,
                        rows_of(buf, nz, region))

    def over_grp(src, buf, number):
        return Exchange(ng, g, lambda p: {"grp": p}, src, lambda k: buf.at[k], number, rows_of(buf, ng, None))

    def quad_index(q):
        return 2 * nz * (q // 2) + 2 * z + q % 2

    def over_quad(src, buf, number):
        return Exchange(4, q_me, lambda p: {"smp": quad_index(p)}, src, lambda k: buf.at[k], number,
                        rows_of(buf, 4, None))

    plane = 4 * g + q_me
    quads = [quad_index(lax.rem(q_me + d, 4)) for d in range(4)]

    def over_all(do):
        for index in quads[1:]:
            do({"grp": g, "smp": index})

        def step(j, carry):
            h = lax.rem(g + j, ng)
            for index in quads:
                do({"grp": h, "smp": index})
            return carry
        lax.fori_loop(1, ng, step, 0)

    class Plane:
        def __init__(self, src, buf, number):
            self.src, self.buf, self.number = src, buf, number
            self.region = buf.at[pl.ds(0, 4 * ng - 1)]

        def start(self):
            over_all(lambda dev: remote(self.src, self.buf.at[plane], send.at[self.number], recv.at[self.number],
                                        dev).start())

        def wait(self):
            all_of(self.region, self.number, False)

        def drain(self):
            all_of(self.region, self.number, True)

    def lane(k, width=LANES):
        return pl.ds(k * width if isinstance(k, int) else pl.multiple_of(k * width, width), width)

    def block(k, size=32):
        return pl.ds(pl.multiple_of(k * size, size), size)

    loads = [pltpu.make_async_copy(a, b, local_sem.at[i]) for i, (a, b) in enumerate(
        ((spk_h, spk), (w_h.at[:, lane(z)], wv), (hb_h, hb), (fb_h, fb), (fw_h, fw)))]
    for load in loads:
        load.start()
    barrier = pltpu.get_barrier_semaphore()
    peers(nz, z, lambda p: pl.semaphore_signal(barrier, inc=1, device_id={"smp": z_index(p)}, device_id_type=MESH))
    over_all(lambda dev: pl.semaphore_signal(barrier, inc=1, device_id=dev, device_id_type=MESH))

    ex_v1 = over_grp(lambda p: vbuf.at[p], v1, 1)
    ex_v2 = over_z(lambda p: v2s, v2, 2)
    ex_v3 = over_grp(lambda p: v3s, v3, 3)
    ex_w1 = over_grp(lambda p: vbuf.at[nz + p], w1, 4)
    ex_w2 = over_z(lambda p: w2s, w2, 5)
    ex_w3 = Plane(w3s, w3, 6)
    ex_p1 = over_grp(lambda p: p1s, p1, 7)
    ex_p2 = over_z(lambda p: p2s, p2, 8)
    ex_p3 = over_quad(lambda p: p3s, p3, 9)
    ex_n1 = Plane(n1s, n1, 10)
    ex_n2 = over_z(lambda p: n2s, n2, 11)
    ex_b1 = over_quad(lambda p: b1s, b1, 12)
    ex_b2 = over_z(lambda p: b2s, b2, 13)
    ex_m1 = Plane(m1s, m1, 29)
    ex_x2 = Plane(x2s, x2, 14)
    ex_x3 = over_z(lambda p: x3s, x3, 30)
    ex_gz = over_z(lambda p: gall.at[q_me, block(p)], gown, 15, lambda k: gown.at[:, lane(k)],
                   gown.at[:, pl.ds(0, LANES * (nz - 1))])

    def gather(buf, first, sems):
        to_core = remote(buf.at[q_me], buf.at[q_me], send.at[first], sems.at[0], {"smp": core})
        to_x = remote(buf.at[q_me], buf.at[q_me], send.at[first + 1], sems.at[1], {"smp": across})
        on = remote(buf.at[q_x], buf.at[q_x], send.at[first + 2], sems.at[2], {"smp": core})
        from_core = remote(buf.at[q_core], buf.at[q_core], send.at[first], sems.at[0], {"smp": core})
        from_x = remote(buf.at[q_x], buf.at[q_x], send.at[first + 1], sems.at[1], {"smp": across})
        from_on = remote(buf.at[q_far], buf.at[q_far], send.at[first + 2], sems.at[2], {"smp": core})
        return to_core, to_x, on, from_core, from_x, from_on

    fx = gather(fc, 16, fx_sem)

    piece = tok // ng
    up, down = lax.rem(z + 1, nz), lax.rem(z + nz - 1, nz)
    near = [remote(spk, pk.at[z], send.at[22 + i], near_sem.at[i], {"smp": z_index(k)})
            for i, k in enumerate((up, down))]
    from_near = [remote(spk, pk.at[k], send.at[22 + i], near_sem.at[i], {"smp": z_index(up)})
                 for i, k in enumerate((down, up))]

    def force_out(k):
        return remote(fw.at[:, lane(k)], fc.at[q_me, block(z)], send.at[0], fa_sem.at[z], {"smp": z_index(k)})

    def force_in(k):
        part = fc.at[q_me, block(k)]
        return remote(part, part, send.at[0], fa_sem.at[k], {"smp": z_index(k)})

    def force_on(k):
        part = fc.at[q_me, block(k)]
        remote(part, part, send.at[17], fx_sem.at[1], {"smp": across}).start()
        remote(part, part, send.at[16], fx_sem.at[0], {"smp": core}).start()

    def far_out(k):
        return remote(spk.at[:, lane(g, piece)], pk.at[z, :, lane(g, piece)], send.at[24], out_sem.at[z],
                      {"smp": z_index(k)})

    def far_first(k):
        part = pk.at[k, :, lane(g, piece)]
        return remote(part, part, send.at[24], out_sem.at[k], {"smp": z_index(k)})

    def far_on(k, h):
        part = pk.at[k, :, lane(g, piece)]
        return remote(part, part, send.at[25], on_sem.at[k], {"grp": h})

    def far_rest(k):
        part = pk.at[k, :, pl.ds(0, piece * (ng - 1))]
        return remote(part, part, send.at[25], on_sem.at[k], {"smp": core})

    bit = jnp.left_shift(jnp.int32(1), lax.broadcasted_iota(jnp.int32, (16, tok), 0)).astype(jnp.int16)

    def unpack(words, j):
        for xq in range(2):
            for cq in range(2):
                for k in range(nz):
                    row = words[pl.ds(2 * nz * xq + 2 * k + cq, 1), :]
                    at = ((2 * xq + cq) * nz + k) * 32
                    for half in range(2):
                        word = jnp.right_shift(row, 16 * half) if half else row
                        word = jnp.broadcast_to(word, (16, tok)).astype(jnp.int16)
                        sgn[pl.ds(at + 16 * half, 16), lane(j, tok)] = jnp.where(
                            jnp.bitwise_and(word, bit) != 0, BF16(1), BF16(-1))

    def hidden(j):
        pre = jnp.dot(wt[...], sgn[:, lane(j, tok)], preferred_element_type=F32)
        for r in range(tiles):
            part = pre[:, r * LANES : (r + 1) * LANES] + cols[0]
            hid[:, lane(j * tiles + r)] = jnp.tanh(part)

    loads[0].wait()
    unpack(spk, 0)
    loads[1].wait()
    loads[2].wait()
    loads[3].wait()
    cols[0] = jnp.broadcast_to(hb[pl.ds(z, 1), :], (LANES, LANES)).T
    cols[1] = jnp.broadcast_to(fb[pl.ds(z, 1), :], (LANES, LANES)).T
    for q in range(4):
        parts = [wv[pl.ds(32 * (2 * nz * (q // 2) + 2 * k + q % 2), 32), :] for k in range(nz)]
        wt[:, q * height : (q + 1) * height] = jnp.concatenate(parts, axis=0).astype(F32).T.astype(BF16)
    loads[4].wait()
    n1s[...] = row_of(folded(fw[...] * fw[...]) + folded(fb[...] * fb[...]) * F32(1.0 / ns))

    pl.semaphore_wait(barrier, nz - 1 + 4 * ng - 1)
    peers(nz, z, lambda k: force_out(k).start())
    peers(nz, z, lambda k: far_out(k).start(), 2, nz - 1)
    for move in near:
        move.start()
    fc[q_me, block(z), :] = fw[:, lane(z)]
    hidden(0)
    ex_n1.start()
    n1[plane] = n1s[...]
    def shard(j):
        d = (j + 1) // 2
        return lax.rem(z + (2 * (j % 2) - 1) * d + nz, nz)

    def each(low, high, act):
        def step(j, carry):
            act(j)
            return carry
        lax.fori_loop(low, high, step, 0)

    once = (s + ns) // ns

    force_on(z)

    def force_pass(j):
        force_in(shard(j)).wait_recv()
        force_on(shard(j))

    each(1, nz, force_pass)

    def pass_on(j):
        k = shard(j)
        far_first(k).wait_recv()
        peers(ng, g, lambda h: far_on(k, h).start())

    each(3, nz, pass_on)

    def transposed(buf, q):
        hi, lo = split(buf[q].T)
        ft[:LANES, lane(q, height)] = hi
        ft[LANES:, lane(q, height)] = lo

    def values(slot, wide, base, col, rows, more=False):
        span = pl.ds(slot * tok, wide * tok)
        res = jnp.dot(ft[:, rows], sgn[rows, span], preferred_element_type=F32)
        for n in range(wide):
            k = shard(slot + n)
            for r in range(tiles):
                at = (n * tiles + r) * LANES
                both = res[:LANES, at : at + LANES] + res[LANES:, at : at + LANES]
                if col is not None:
                    both = both + cols[col]
                got = row_of(both * hid[:, lane((slot + n) * tiles + r)])
                to = (base + k, pl.ds(r, 1), slice(None))
                vbuf[to] = vbuf[to] + got if more else got

    for i in (1, 0):
        from_near[i].wait_recv()
        unpack(pk.at[(down, up)[i]], 2 - i)
        hidden(2 - i)
    def arrive(j):
        k = shard(j)
        far_rest(k).wait_recv()
        unpack(pk.at[k], j)
        hidden(j)

    fx[4].wait_recv()
    fx[2].start()
    fx[3].wait_recv()
    transposed(fc, q_me)
    transposed(fc, q_core)
    transposed(fc, q_x)
    early = 3 if nz == 4 else 5
    each(3, early, arrive)
    fx[5].wait_recv()
    transposed(fc, q_far)
    every = pl.ds(0, 4 * height)
    values(0, 3, 0, 1, every)
    for j in range(early, nz):
        far_rest(shard(j)).wait_recv()

    def overlap(_):
        for j in range(early, nz):
            unpack(pk.at[shard(j)], j)
            if j == early and early > 3:
                values(3, early - 3, 0, 1, every)
            hidden(j)

    each(0, once, overlap)
    values(early, nz - early, 0, 1, every)

    ex_v1.start()
    p1s[...] = row_of(added([vbuf[k] for k in range(nz)]))
    ex_p1.start()
    v1[g] = vbuf[g]
    p1[g] = p1s[...]
    ex_n1.wait()
    n2s[...] = added([n1[k] for k in range(4 * ng)])
    ex_n2.start()
    n2[z] = n2s[...]
    ex_v1.wait()
    v2s[...] = added([v1[k] for k in range(ng)])
    ex_v2.start()
    ex_p1.wait()
    p2s[...] = added([p1[k] for k in range(ng)])
    ex_p2.start()
    v2[z] = v2s[...]
    p2[z] = p2s[...]
    peers(nz, z, lambda k: force_out(k).wait_send())
    ex_v1.drain()
    ex_p1.drain()
    ex_n1.drain()
    for move in near:
        move.wait_send()
    peers(nz, z, lambda k: far_out(k).wait_send(), 2, nz - 1)
    ex_v2.wait()
    v3s[...] = added([v2[k] for k in range(nz)])
    ex_v3.start()
    ex_p2.wait()
    p3s[...] = added([p2[k] for k in range(nz)])
    ex_p3.start()
    v3[g] = v3s[...]
    p3[q_me] = p3s[...]
    ex_v2.drain()
    ex_p2.drain()
    peers(nz, z, lambda k: far_rest(k).wait_send(), 2, nz - 1)
    ex_v3.wait()
    ex_p3.wait()
    inv = F32(1.0 / count)
    mean = total(added([p3[k] for k in range(4)])) * inv
    mine = (c, 2 + c)
    other = (1 - c, 3 - c)

    def first_rows(_):
        bias = jnp.zeros((LANES, LANES), F32)
        sums = [None, None]
        for j in range(nz):
            own = v3[shard(j)] - mean
            for r in range(tiles):
                at = (j * tiles + r) * LANES
                prod = hid[:, at : at + LANES] * own[r : r + 1, :]
                hi, lo = split(prod)
                ch[:LANES, at : at + LANES] = hi
                ch[LANES:, at : at + LANES] = lo
                bias = bias + prod
            span = slice(j * tok, (j + 1) * tok)
            res = lax.dot_general(sgn[block(other[0], height), span], ch[:, span],
                                  (((1,), (1,)), ((), ())), preferred_element_type=F32)
            sums[j % 2] = res if j < 2 else sums[j % 2] + res
        res = sums[0] + sums[1]
        gi[other[0]] = res[:, :LANES] + res[:, LANES:]
        gb[...] = bias

    each(0, once, first_rows)

    def image(q):
        def run(_):
            res = lax.dot_general(sgn[block(q, height), :], ch[...], (((1,), (1,)), ((), ())),
                                  preferred_element_type=F32)
            gi[q] = res[:, :LANES] + res[:, LANES:]
        each(0, once, run)

    to_core = [remote(gi.at[other[i]], rs_r.at[i], send.at[26 + i], rs_sem.at[i], {"smp": core}) for i in range(2)]
    to_x = [remote(rs_s.at[i], rs_r.at[2 + i], send.at[19 + i], rs_sem.at[2 + i], {"smp": across}) for i in range(2)]
    share = [remote(gall.at[mine[i]], gall.at[mine[i]], send.at[21 + 7 * i], ag_sem.at[i], {"smp": core})
             for i in range(2)]
    shared = [remote(gall.at[other[i]], gall.at[other[i]], send.at[21 + 7 * i], ag_sem.at[i], {"smp": core})
              for i in range(2)]
    to_core[0].start()
    b1s[...] = row_of(gb[...].T)
    off = v3s[...] - mean
    m1s[...] = row_of(off * off)
    ex_b1.start()
    b1[q_me] = b1s[...]
    image(mine[0])
    to_core[0].wait_recv()
    rs_s[0] = gi[mine[0]] + rs_r[0]
    to_x[0].start()
    ex_m1.start()
    m1[plane] = m1s[...]
    image(other[1])
    to_core[1].start()
    image(mine[1])
    to_core[1].wait_recv()
    rs_s[1] = gi[mine[1]] + rs_r[1]
    to_x[1].start()
    ex_v3.drain()
    ex_p3.drain()
    ex_n2.wait()
    ex_n2.drain()
    norm0 = total(added([n2[k] for k in range(nz)]))
    ex_b1.wait()
    b2s[...] = added([b1[k] for k in range(4)])
    ex_b2.start()
    b2[z] = b2s[...]
    cols[2] = jnp.broadcast_to(b2s[...], (LANES, LANES)).T
    ex_b1.drain()

    def quarter(q, first=False):
        transposed(gall, q)
        each(0, once, lambda i: values(0, nz, nz, 2 if first else None, block(q, height), not first))

    to_x[0].wait_recv()
    gall[mine[0]] = rs_s[0] + rs_r[2]
    share[0].start()
    quarter(mine[0], True)
    shared[0].wait_recv()
    quarter(other[0])
    ex_b2.wait()
    ex_m1.wait()
    for k in range(nz):
        gb[pl.ds(k, 1), :] = b2[k]
    if nz < 8:
        gb[nz:8, :] = jnp.zeros((8 - nz, LANES), F32)
    image_b = gb[:8, :]
    curvature = total(added([m1[k] for k in range(4 * ng)])) * inv + F32(LAMBDA) * norm0
    alpha0 = norm0 / curvature
    to_x[1].wait_recv()
    gall[mine[1]] = rs_s[1] + rs_r[3]
    share[1].start()
    ex_gz.start()
    gown[:, lane(z)] = gall[q_me, block(z), :]

    res_b = fb[...] - alpha0 * (image_b * inv + F32(LAMBDA) * fb[...])
    own_f = fc[q_me]
    res_w = own_f - alpha0 * (gall[q_me] * inv + F32(LAMBDA) * own_f)
    x2s[0:1] = row_of(folded(res_w * res_w) + res_b * res_b * F32(1.0 / ns))
    x2s[1:2] = row_of(folded(res_w * own_f) + res_b * fb[...] * F32(1.0 / ns))
    ex_x2.start()
    x2[plane] = x2s[...]
    quarter(mine[1])
    shared[1].wait_recv()
    quarter(other[1])

    ex_w1.start()
    w1[g] = vbuf[nz + g]
    ex_x2.wait()
    x3s[...] = added([x2[k] for k in range(4 * ng)])
    ex_x3.start()
    x3[z] = x3s[...]
    for move in (*fx[:3], *to_core, *to_x, *share):
        move.wait_send()
    for ex in (ex_m1, ex_b2, ex_gz):
        ex.drain()
    ex_gz.wait()
    ex_w1.wait()
    w2s[...] = added([w1[k] for k in range(ng)])
    ex_w2.start()
    w2[z] = w2s[...]
    ex_w1.drain()
    ex_x2.drain()
    ex_x3.wait()
    ex_x3.drain()
    sums = added([x3[k] for k in range(nz)])
    norm1 = total(sums[0:1])
    cross = total(sums[1:2])
    beta = norm1 / norm0
    scale_f = F32(1.0) - alpha0 * F32(LAMBDA) + beta
    norm_d = norm1 + F32(2.0) * beta * cross + beta * beta * norm0
    ex_w2.wait()
    mixed = scale_f * off - (alpha0 * inv) * added([w2[k] for k in range(nz)])
    here = total(mixed)
    spread = mixed - here * F32(1.0 / tok)
    w3s[0:1] = jnp.broadcast_to(here, (1, LANES))
    w3s[1:2] = row_of(spread * spread)
    ex_w3.start()
    w3[plane] = w3s[...]
    ex_w2.drain()
    ex_w3.wait()
    shards = [w3[k, 0:1, :] for k in range(4 * ng)]
    mean1 = added(shards) * inv
    between = row_of(jnp.zeros((1, LANES), F32))
    for one in shards:
        gap = one * F32(1.0 / tok) - mean1
        between += gap * gap
    within = total(added([w3[k, 1:2, :] for k in range(4 * ng)]))
    square = within + between[:, 0:1] * F32(tok)
    curvature = square * inv + F32(LAMBDA) * norm_d
    alpha1 = norm1 / curvature
    factor_f = alpha0 + alpha1 * scale_f
    factor_g = alpha1 * alpha0 * inv
    out_w[...] = factor_f * fw[...] - factor_g * gown[...]
    out_b[...] = factor_f * fb[...] - factor_g * image_b
    stores = [pltpu.make_async_copy(a, b, local_sem.at[5 + i]) for i, (a, b) in enumerate(
        ((out_w, out_w_h), (out_b, out_b_h)))]
    for store in stores:
        store.start()
    ex_w3.drain()
    for store in stores:
        store.wait()


def call(ng, nz, count, spk, w, hb, fw, fb):
    ns = 4 * nz
    tok = spk.shape[1]
    words, height = spk.shape[0], 32 * nz
    nv = 32 * words
    tile = (8, LANES)
    dma = pltpu.SemaphoreType.DMA
    anywhere = pl.BlockSpec(memory_space=pl.ANY)

    def f32(*shape):
        return pltpu.VMEM(shape, F32)

    scratch = [
        pltpu.VMEM((words, tok), jnp.int32), f32(*fw.shape), f32(*tile), f32(*tile), f32(*fw.shape), f32(*tile),
        pltpu.VMEM((nz, words, tok), jnp.int32),
        pltpu.VMEM((nv, LANES), BF16),
        pltpu.VMEM((LANES, nv), BF16),
        f32(4, height, LANES),
        pltpu.VMEM((2 * LANES, nv), BF16),
        pltpu.VMEM((nv, nz * tok), BF16),
        f32(LANES, nz * tok),
        pltpu.VMEM((2 * LANES, nz * tok), BF16),
        f32(2 * nz, *tile), f32(ng, *tile), f32(nz, *tile), f32(ng, *tile), f32(*tile), f32(*tile),
        f32(ng, *tile), f32(nz, *tile), f32(*tile),
        f32(1, LANES), f32(ng, 1, LANES), f32(1, LANES), f32(nz, 1, LANES), f32(1, LANES), f32(4, 1, LANES),
        f32(1, LANES), f32(4 * ng, 1, LANES), f32(1, LANES), f32(nz, 1, LANES),
        f32(1, LANES), f32(4, 1, LANES), f32(1, LANES), f32(nz, 1, LANES), f32(1, LANES), f32(4 * ng, 1, LANES),
        f32(2, LANES), f32(4 * ng, 2, LANES), f32(2, LANES), f32(nz, 2, LANES), f32(2, LANES), f32(4 * ng, 2, LANES),
        f32(LANES, LANES), f32(4, height, LANES), f32(2, height, LANES), f32(4, height, LANES), f32(4, height, LANES),
        f32(32, nz * LANES), f32(3, LANES, LANES),
        dma((7,)), dma((31,)), dma((31,)), dma((2,)), dma((nz,)), dma((nz,)), dma((nz,)), dma((3,)), dma((4,)), dma((2,)),
    ]
    return pl.pallas_call(
        functools.partial(kernel, ng, nz, count),
        out_shape=(jax.ShapeDtypeStruct(fw.shape, F32), jax.ShapeDtypeStruct(tile, F32)),
        in_specs=[anywhere] * 5,
        out_specs=(anywhere, anywhere),
        scratch_shapes=scratch,
        compiler_params=pltpu.CompilerParams(collective_id=0, has_side_effects=True,
                                             vmem_limit_bytes=60 * 1024 * 1024),
        name="step",
    )(spk, w, hb, fw, fb)


def solution(mesh):
    ng, ns = mesh.shape["grp"], mesh.shape["smp"]
    nz = ns // 4

    def body(spk, w, hb, fw, fb):
        count = spk.shape[1] * ns
        tile = (8, LANES)
        pad = 8 * LANES - hb.shape[0]
        hb, fb = (jnp.pad(v, (0, pad)).reshape(tile) for v in (hb, fb))
        out_w, out_b = call(ng, nz, count, spk, w, hb, fw, fb)
        return out_w, out_b.reshape(-1)[: nz * LANES]

    return jax.shard_map(body, mesh=mesh,
                         in_specs=(P(None, "smp"), P(None, "grp"), P("grp"), P("smp", "grp"), P("grp")),
                         out_specs=(P("smp", "grp"), P("grp")), check_vma=False)
```

```python
import functools

import jax
import jax.numpy as jnp
from jax import lax
from jax.experimental import pallas as pl
from jax.experimental.pallas import tpu as pltpu
from jax.sharding import PartitionSpec as P

MESH = pl.DeviceIdType.MESH
LAMBDA = 0.01
F32 = jnp.float32
BF16 = jnp.bfloat16
LANES = 128


def split(x):
    hi = x.astype(BF16)
    return hi, (x - hi.astype(F32)).astype(BF16)


def folded(x):
    rows, cols = x.shape
    tiles = [x[r : r + 8, k : k + LANES] for r in range(0, rows, 8) for k in range(0, cols, LANES)]
    return functools.reduce(lambda a, b: a + b, tiles)


def total(x):
    return jnp.sum(jnp.sum(x, axis=0, keepdims=True), axis=1, keepdims=True)


def row_of(x):
    return jnp.sum(x, axis=0, keepdims=True)


def added(parts):
    return functools.reduce(lambda a, b: a + b, parts)


def kernel(ng, nz, count, spk_h, w_h, hb_h, fw_h, fb_h, out_w_h, out_b_h,
           spk, fw, hb, fb, out_w, out_b, pk, wv, wt, fc, ft, sgn, hid, ch,
           vbuf, v1, v2, v3, v2s, v3s, w1, w2, w2s,
           p1s, p1, p2s, p2, p3s, p3, n1s, n1, n2s, n2, b1s, b1, b2s, b2, m1s, m1, x2s, x2, x3s, x3, w3s, w3,
           gb, gi, rs_s, rs_r, gall, gown, cols,
           local_sem, send, recv, near_sem, fa_sem, out_sem, on_sem, fx_sem, rs_sem, ag_sem):
    ns = 4 * nz
    tok = spk.shape[1]
    tiles = tok // LANES
    height = 32 * nz
    s = lax.axis_index("smp")
    g = lax.axis_index("grp")
    xh = s // (2 * nz)
    z = (s // 2) % nz
    c = s % 2
    q_me = 2 * xh + c
    q_core = 2 * xh + 1 - c
    q_x = 2 * (1 - xh) + c
    q_far = 2 * (1 - xh) + 1 - c
    core = s + 1 - 2 * c
    across = s + (2 * nz) * (1 - 2 * xh)

    def z_index(k):
        return 2 * nz * xh + 2 * k + c

    def remote(src, dst, ssem, rsem, dev):
        return pltpu.make_async_remote_copy(src_ref=src, dst_ref=dst, send_sem=ssem, recv_sem=rsem,
                                            device_id=dev, device_id_type=MESH)

    def peers(n, me, act, low=1, high=None):
        def step(j, carry):
            act(lax.rem(me + j, n))
            return carry
        lax.fori_loop(low, n if high is None else high, step, 0)

    def all_of(region, number, sent):
        move = remote(region, region, send.at[number], recv.at[number], {"smp": core})
        move.wait_send() if sent else move.wait_recv()

    class Exchange:
        def __init__(self, n, me, dev, src, dst, number, region):
            self.n, self.me, self.dev, self.src, self.dst = n, me, dev, src, dst
            self.number, self.region = number, region

        def start(self):
            peers(self.n, self.me, lambda p: remote(self.src(p), self.dst(self.me), send.at[self.number],
                                                    recv.at[self.number], self.dev(p)).start())

        def wait(self):
            all_of(self.region, self.number, False)

        def drain(self):
            all_of(self.region, self.number, True)

    def rows_of(buf, n, dst):
        return buf.at[pl.ds(0, n - 1)] if dst is None else dst

    def over_z(src, buf, number, dst=None, region=None):
        return Exchange(nz, z, lambda p: {"smp": z_index(p)}, src, dst or (lambda k: buf.at[k]), number,
                        rows_of(buf, nz, region))

    def over_grp(src, buf, number):
        return Exchange(ng, g, lambda p: {"grp": p}, src, lambda k: buf.at[k], number, rows_of(buf, ng, None))

    def quad_index(q):
        return 2 * nz * (q // 2) + 2 * z + q % 2

    def over_quad(src, buf, number):
        return Exchange(4, q_me, lambda p: {"smp": quad_index(p)}, src, lambda k: buf.at[k], number,
                        rows_of(buf, 4, None))

    plane = 4 * g + q_me
    quads = [quad_index(lax.rem(q_me + d, 4)) for d in range(4)]

    def over_all(do):
        for index in quads[1:]:
            do({"grp": g, "smp": index})

        def step(j, carry):
            h = lax.rem(g + j, ng)
            for index in quads:
                do({"grp": h, "smp": index})
            return carry
        lax.fori_loop(1, ng, step, 0)

    class Plane:
        def __init__(self, src, buf, number):
            self.src, self.buf, self.number = src, buf, number
            self.region = buf.at[pl.ds(0, 4 * ng - 1)]

        def start(self):
            over_all(lambda dev: remote(self.src, self.buf.at[plane], send.at[self.number], recv.at[self.number],
                                        dev).start())

        def wait(self):
            all_of(self.region, self.number, False)

        def drain(self):
            all_of(self.region, self.number, True)

    def lane(k, width=LANES):
        return pl.ds(k * width if isinstance(k, int) else pl.multiple_of(k * width, width), width)

    def block(k, size=32):
        return pl.ds(pl.multiple_of(k * size, size), size)

    loads = [pltpu.make_async_copy(a, b, local_sem.at[i]) for i, (a, b) in enumerate(
        ((spk_h, spk), (w_h.at[:, lane(z)], wv), (hb_h, hb), (fb_h, fb), (fw_h, fw)))]
    for load in loads:
        load.start()
    barrier = pltpu.get_barrier_semaphore()
    peers(nz, z, lambda p: pl.semaphore_signal(barrier, inc=1, device_id={"smp": z_index(p)}, device_id_type=MESH))
    over_all(lambda dev: pl.semaphore_signal(barrier, inc=1, device_id=dev, device_id_type=MESH))

    ex_v1 = over_grp(lambda p: vbuf.at[p], v1, 1)
    ex_v2 = over_z(lambda p: v2s, v2, 2)
    ex_v3 = over_grp(lambda p: v3s, v3, 3)
    ex_w1 = over_grp(lambda p: vbuf.at[nz + p], w1, 4)
    ex_w2 = over_z(lambda p: w2s, w2, 5)
    ex_w3 = Plane(w3s, w3, 6)
    ex_p1 = over_grp(lambda p: p1s, p1, 7)
    ex_p2 = over_z(lambda p: p2s, p2, 8)
    ex_p3 = over_quad(lambda p: p3s, p3, 9)
    ex_n1 = Plane(n1s, n1, 10)
    ex_n2 = over_z(lambda p: n2s, n2, 11)
    ex_b1 = over_quad(lambda p: b1s, b1, 12)
    ex_b2 = over_z(lambda p: b2s, b2, 13)
    ex_m1 = Plane(m1s, m1, 29)
    ex_x2 = Plane(x2s, x2, 14)
    ex_x3 = over_z(lambda p: x3s, x3, 30)
    ex_gz = over_z(lambda p: gall.at[q_me, block(p)], gown, 15, lambda k: gown.at[:, lane(k)],
                   gown.at[:, pl.ds(0, LANES * (nz - 1))])

    def gather(buf, first, sems):
        to_core = remote(buf.at[q_me], buf.at[q_me], send.at[first], sems.at[0], {"smp": core})
        to_x = remote(buf.at[q_me], buf.at[q_me], send.at[first + 1], sems.at[1], {"smp": across})
        on = remote(buf.at[q_x], buf.at[q_x], send.at[first + 2], sems.at[2], {"smp": core})
        from_core = remote(buf.at[q_core], buf.at[q_core], send.at[first], sems.at[0], {"smp": core})
        from_x = remote(buf.at[q_x], buf.at[q_x], send.at[first + 1], sems.at[1], {"smp": across})
        from_on = remote(buf.at[q_far], buf.at[q_far], send.at[first + 2], sems.at[2], {"smp": core})
        return to_core, to_x, on, from_core, from_x, from_on

    fx = gather(fc, 16, fx_sem)

    piece = tok // ng
    up, down = lax.rem(z + 1, nz), lax.rem(z + nz - 1, nz)
    near = [remote(spk, pk.at[z], send.at[22 + i], near_sem.at[i], {"smp": z_index(k)})
            for i, k in enumerate((up, down))]
    from_near = [remote(spk, pk.at[k], send.at[22 + i], near_sem.at[i], {"smp": z_index(up)})
                 for i, k in enumerate((down, up))]

    def force_out(k):
        return remote(fw.at[:, lane(k)], fc.at[q_me, block(z)], send.at[0], fa_sem.at[z], {"smp": z_index(k)})

    def force_in(k):
        part = fc.at[q_me, block(k)]
        return remote(part, part, send.at[0], fa_sem.at[k], {"smp": z_index(k)})

    def force_on(k):
        part = fc.at[q_me, block(k)]
        remote(part, part, send.at[17], fx_sem.at[1], {"smp": across}).start()
        remote(part, part, send.at[16], fx_sem.at[0], {"smp": core}).start()

    def far_out(k):
        return remote(spk.at[:, lane(g, piece)], pk.at[z, :, lane(g, piece)], send.at[24], out_sem.at[z],
                      {"smp": z_index(k)})

    def far_first(k):
        part = pk.at[k, :, lane(g, piece)]
        return remote(part, part, send.at[24], out_sem.at[k], {"smp": z_index(k)})

    def far_on(k, h):
        part = pk.at[k, :, lane(g, piece)]
        return remote(part, part, send.at[25], on_sem.at[k], {"grp": h})

    def far_rest(k):
        part = pk.at[k, :, pl.ds(0, piece * (ng - 1))]
        return remote(part, part, send.at[25], on_sem.at[k], {"smp": core})

    bit = jnp.left_shift(jnp.int32(1), lax.broadcasted_iota(jnp.int32, (16, tok), 0)).astype(jnp.int16)

    def unpack(words, j):
        for xq in range(2):
            for cq in range(2):
                for k in range(nz):
                    row = words[pl.ds(2 * nz * xq + 2 * k + cq, 1), :]
                    at = ((2 * xq + cq) * nz + k) * 32
                    for half in range(2):
                        word = jnp.right_shift(row, 16 * half) if half else row
                        word = jnp.broadcast_to(word, (16, tok)).astype(jnp.int16)
                        sgn[pl.ds(at + 16 * half, 16), lane(j, tok)] = jnp.where(
                            jnp.bitwise_and(word, bit) != 0, BF16(1), BF16(-1))

    def hidden(j):
        pre = jnp.dot(wt[...], sgn[:, lane(j, tok)], preferred_element_type=F32)
        for r in range(tiles):
            part = pre[:, r * LANES : (r + 1) * LANES] + cols[0]
            hid[:, lane(j * tiles + r)] = jnp.tanh(part)

    loads[0].wait()
    unpack(spk, 0)
    loads[1].wait()
    loads[2].wait()
    loads[3].wait()
    cols[0] = jnp.broadcast_to(hb[pl.ds(z, 1), :], (LANES, LANES)).T
    cols[1] = jnp.broadcast_to(fb[pl.ds(z, 1), :], (LANES, LANES)).T
    for q in range(4):
        parts = [wv[pl.ds(32 * (2 * nz * (q // 2) + 2 * k + q % 2), 32), :] for k in range(nz)]
        wt[:, q * height : (q + 1) * height] = jnp.concatenate(parts, axis=0).astype(F32).T.astype(BF16)
    loads[4].wait()
    n1s[...] = row_of(folded(fw[...] * fw[...]) + folded(fb[...] * fb[...]) * F32(1.0 / ns))

    pl.semaphore_wait(barrier, nz - 1 + 4 * ng - 1)
    peers(nz, z, lambda k: force_out(k).start())
    peers(nz, z, lambda k: far_out(k).start(), 2, nz - 1)
    for move in near:
        move.start()
    fc[q_me, block(z), :] = fw[:, lane(z)]
    hidden(0)
    ex_n1.start()
    n1[plane] = n1s[...]
    def shard(j):
        d = (j + 1) // 2
        return lax.rem(z + (2 * (j % 2) - 1) * d + nz, nz)

    def each(low, high, act):
        def step(j, carry):
            act(j)
            return carry
        lax.fori_loop(low, high, step, 0)

    once = (s + ns) // ns

    force_on(z)

    def force_pass(j):
        force_in(shard(j)).wait_recv()
        force_on(shard(j))

    each(1, nz, force_pass)

    def pass_on(j):
        k = shard(j)
        far_first(k).wait_recv()
        peers(ng, g, lambda h: far_on(k, h).start())

    each(3, nz, pass_on)

    def transposed(buf, q):
        hi, lo = split(buf[q].T)
        ft[:LANES, lane(q, height)] = hi
        ft[LANES:, lane(q, height)] = lo

    def values(slot, wide, base, col, rows, more=False):
        span = pl.ds(slot * tok, wide * tok)
        res = jnp.dot(ft[:, rows], sgn[rows, span], preferred_element_type=F32)
        for n in range(wide):
            k = shard(slot + n)
            for r in range(tiles):
                at = (n * tiles + r) * LANES
                both = res[:LANES, at : at + LANES] + res[LANES:, at : at + LANES]
                if col is not None:
                    both = both + cols[col]
                got = row_of(both * hid[:, lane((slot + n) * tiles + r)])
                to = (base + k, pl.ds(r, 1), slice(None))
                vbuf[to] = vbuf[to] + got if more else got

    for i in (1, 0):
        from_near[i].wait_recv()
        unpack(pk.at[(down, up)[i]], 2 - i)
        hidden(2 - i)
    def arrive(j):
        k = shard(j)
        far_rest(k).wait_recv()
        unpack(pk.at[k], j)
        hidden(j)

    fx[4].wait_recv()
    fx[2].start()
    fx[3].wait_recv()
    transposed(fc, q_me)
    transposed(fc, q_core)
    transposed(fc, q_x)
    early = 3 if nz == 4 else 5
    each(3, early, arrive)
    fx[5].wait_recv()
    transposed(fc, q_far)
    every = pl.ds(0, 4 * height)
    values(0, 3, 0, 1, every)
    for j in range(early, nz):
        far_rest(shard(j)).wait_recv()

    def overlap(_):
        for j in range(early, nz):
            unpack(pk.at[shard(j)], j)
            if j == early and early > 3:
                values(3, early - 3, 0, 1, every)
            hidden(j)

    each(0, once, overlap)
    values(early, nz - early, 0, 1, every)

    ex_v1.start()
    p1s[...] = row_of(added([vbuf[k] for k in range(nz)]))
    ex_p1.start()
    v1[g] = vbuf[g]
    p1[g] = p1s[...]
    ex_n1.wait()
    n2s[...] = added([n1[k] for k in range(4 * ng)])
    ex_n2.start()
    n2[z] = n2s[...]
    ex_v1.wait()
    v2s[...] = added([v1[k] for k in range(ng)])
    ex_v2.start()
    ex_p1.wait()
    p2s[...] = added([p1[k] for k in range(ng)])
    ex_p2.start()
    v2[z] = v2s[...]
    p2[z] = p2s[...]
    peers(nz, z, lambda k: force_out(k).wait_send())
    ex_v1.drain()
    ex_p1.drain()
    ex_n1.drain()
    for move in near:
        move.wait_send()
    peers(nz, z, lambda k: far_out(k).wait_send(), 2, nz - 1)
    ex_v2.wait()
    v3s[...] = added([v2[k] for k in range(nz)])
    ex_v3.start()
    ex_p2.wait()
    p3s[...] = added([p2[k] for k in range(nz)])
    ex_p3.start()
    v3[g] = v3s[...]
    p3[q_me] = p3s[...]
    ex_v2.drain()
    ex_p2.drain()
    peers(nz, z, lambda k: far_rest(k).wait_send(), 2, nz - 1)
    ex_v3.wait()
    ex_p3.wait()
    inv = F32(1.0 / count)
    mean = total(added([p3[k] for k in range(4)])) * inv
    mine = (c, 2 + c)
    other = (1 - c, 3 - c)

    def first_rows(_):
        bias = jnp.zeros((LANES, LANES), F32)
        sums = [None, None]
        for j in range(nz):
            own = v3[shard(j)] - mean
            for r in range(tiles):
                at = (j * tiles + r) * LANES
                prod = hid[:, at : at + LANES] * own[r : r + 1, :]
                hi, lo = split(prod)
                ch[:LANES, at : at + LANES] = hi
                ch[LANES:, at : at + LANES] = lo
                bias = bias + prod
            span = slice(j * tok, (j + 1) * tok)
            res = lax.dot_general(sgn[block(other[0], height), span], ch[:, span],
                                  (((1,), (1,)), ((), ())), preferred_element_type=F32)
            sums[j % 2] = res if j < 2 else sums[j % 2] + res
        res = sums[0] + sums[1]
        gi[other[0]] = res[:, :LANES] + res[:, LANES:]
        gb[...] = bias

    each(0, once, first_rows)

    def image(q):
        def run(_):
            res = lax.dot_general(sgn[block(q, height), :], ch[...], (((1,), (1,)), ((), ())),
                                  preferred_element_type=F32)
            gi[q] = res[:, :LANES] + res[:, LANES:]
        each(0, once, run)

    to_core = [remote(gi.at[other[i]], rs_r.at[i], send.at[26 + i], rs_sem.at[i], {"smp": core}) for i in range(2)]
    to_x = [remote(rs_s.at[i], rs_r.at[2 + i], send.at[19 + i], rs_sem.at[2 + i], {"smp": across}) for i in range(2)]
    share = [remote(gall.at[mine[i]], gall.at[mine[i]], send.at[21 + 7 * i], ag_sem.at[i], {"smp": core})
             for i in range(2)]
    shared = [remote(gall.at[other[i]], gall.at[other[i]], send.at[21 + 7 * i], ag_sem.at[i], {"smp": core})
              for i in range(2)]
    to_core[0].start()
    b1s[...] = row_of(gb[...].T)
    off = v3s[...] - mean
    m1s[...] = row_of(off * off)
    ex_b1.start()
    b1[q_me] = b1s[...]
    image(mine[0])
    to_core[0].wait_recv()
    rs_s[0] = gi[mine[0]] + rs_r[0]
    to_x[0].start()
    ex_m1.start()
    m1[plane] = m1s[...]
    image(other[1])
    to_core[1].start()
    image(mine[1])
    to_core[1].wait_recv()
    rs_s[1] = gi[mine[1]] + rs_r[1]
    to_x[1].start()
    ex_v3.drain()
    ex_p3.drain()
    ex_n2.wait()
    ex_n2.drain()
    norm0 = total(added([n2[k] for k in range(nz)]))
    ex_b1.wait()
    b2s[...] = added([b1[k] for k in range(4)])
    ex_b2.start()
    b2[z] = b2s[...]
    cols[2] = jnp.broadcast_to(b2s[...], (LANES, LANES)).T
    ex_b1.drain()

    def quarter(q, first=False):
        transposed(gall, q)
        each(0, once, lambda i: values(0, nz, nz, 2 if first else None, block(q, height), not first))

    to_x[0].wait_recv()
    gall[mine[0]] = rs_s[0] + rs_r[2]
    share[0].start()
    quarter(mine[0], True)
    shared[0].wait_recv()
    quarter(other[0])
    ex_b2.wait()
    ex_m1.wait()
    for k in range(nz):
        gb[pl.ds(k, 1), :] = b2[k]
    if nz < 8:
        gb[nz:8, :] = jnp.zeros((8 - nz, LANES), F32)
    image_b = gb[:8, :]
    curvature = total(added([m1[k] for k in range(4 * ng)])) * inv + F32(LAMBDA) * norm0
    alpha0 = norm0 / curvature
    to_x[1].wait_recv()
    gall[mine[1]] = rs_s[1] + rs_r[3]
    share[1].start()
    ex_gz.start()
    gown[:, lane(z)] = gall[q_me, block(z), :]

    res_b = fb[...] - alpha0 * (image_b * inv + F32(LAMBDA) * fb[...])
    own_f = fc[q_me]
    res_w = own_f - alpha0 * (gall[q_me] * inv + F32(LAMBDA) * own_f)
    x2s[0:1] = row_of(folded(res_w * res_w) + res_b * res_b * F32(1.0 / ns))
    x2s[1:2] = row_of(folded(res_w * own_f) + res_b * fb[...] * F32(1.0 / ns))
    ex_x2.start()
    x2[plane] = x2s[...]
    quarter(mine[1])
    shared[1].wait_recv()
    quarter(other[1])

    ex_w1.start()
    w1[g] = vbuf[nz + g]
    ex_x2.wait()
    x3s[...] = added([x2[k] for k in range(4 * ng)])
    ex_x3.start()
    x3[z] = x3s[...]
    for move in (*fx[:3], *to_core, *to_x, *share):
        move.wait_send()
    for ex in (ex_m1, ex_b2, ex_gz):
        ex.drain()
    ex_gz.wait()
    ex_w1.wait()
    w2s[...] = added([w1[k] for k in range(ng)])
    ex_w2.start()
    w2[z] = w2s[...]
    ex_w1.drain()
    ex_x2.drain()
    ex_x3.wait()
    ex_x3.drain()
    sums = added([x3[k] for k in range(nz)])
    norm1 = total(sums[0:1])
    cross = total(sums[1:2])
    beta = norm1 / norm0
    scale_f = F32(1.0) - alpha0 * F32(LAMBDA) + beta
    norm_d = norm1 + F32(2.0) * beta * cross + beta * beta * norm0
    ex_w2.wait()
    mixed = scale_f * off - (alpha0 * inv) * added([w2[k] for k in range(nz)])
    here = total(mixed)
    spread = mixed - here * F32(1.0 / tok)
    w3s[0:1] = jnp.broadcast_to(here, (1, LANES))
    w3s[1:2] = row_of(spread * spread)
    ex_w3.start()
    w3[plane] = w3s[...]
    ex_w2.drain()
    ex_w3.wait()
    shards = [w3[k, 0:1, :] for k in range(4 * ng)]
    mean1 = added(shards) * inv
    between = row_of(jnp.zeros((1, LANES), F32))
    for one in shards:
        gap = one * F32(1.0 / tok) - mean1
        between += gap * gap
    within = total(added([w3[k, 1:2, :] for k in range(4 * ng)]))
    square = within + between[:, 0:1] * F32(tok)
    curvature = square * inv + F32(LAMBDA) * norm_d
    alpha1 = norm1 / curvature
    factor_f = alpha0 + alpha1 * scale_f
    factor_g = alpha1 * alpha0 * inv
    out_w[...] = factor_f * fw[...] - factor_g * gown[...]
    out_b[...] = factor_f * fb[...] - factor_g * image_b
    stores = [pltpu.make_async_copy(a, b, local_sem.at[5 + i]) for i, (a, b) in enumerate(
        ((out_w, out_w_h), (out_b, out_b_h)))]
    for store in stores:
        store.start()
    ex_w3.drain()
    for store in stores:
        store.wait()


def call(ng, nz, count, spk, w, hb, fw, fb):
    ns = 4 * nz
    tok = spk.shape[1]
    words, height = spk.shape[0], 32 * nz
    nv = 32 * words
    tile = (8, LANES)
    dma = pltpu.SemaphoreType.DMA
    anywhere = pl.BlockSpec(memory_space=pl.ANY)

    def f32(*shape):
        return pltpu.VMEM(shape, F32)

    scratch = [
        pltpu.VMEM((words, tok), jnp.int32), f32(*fw.shape), f32(*tile), f32(*tile), f32(*fw.shape), f32(*tile),
        pltpu.VMEM((nz, words, tok), jnp.int32),
        pltpu.VMEM((nv, LANES), BF16),
        pltpu.VMEM((LANES, nv), BF16),
        f32(4, height, LANES),
        pltpu.VMEM((2 * LANES, nv), BF16),
        pltpu.VMEM((nv, nz * tok), BF16),
        f32(LANES, nz * tok),
        pltpu.VMEM((2 * LANES, nz * tok), BF16),
        f32(2 * nz, *tile), f32(ng, *tile), f32(nz, *tile), f32(ng, *tile), f32(*tile), f32(*tile),
        f32(ng, *tile), f32(nz, *tile), f32(*tile),
        f32(1, LANES), f32(ng, 1, LANES), f32(1, LANES), f32(nz, 1, LANES), f32(1, LANES), f32(4, 1, LANES),
        f32(1, LANES), f32(4 * ng, 1, LANES), f32(1, LANES), f32(nz, 1, LANES),
        f32(1, LANES), f32(4, 1, LANES), f32(1, LANES), f32(nz, 1, LANES), f32(1, LANES), f32(4 * ng, 1, LANES),
        f32(2, LANES), f32(4 * ng, 2, LANES), f32(2, LANES), f32(nz, 2, LANES), f32(2, LANES), f32(4 * ng, 2, LANES),
        f32(LANES, LANES), f32(4, height, LANES), f32(2, height, LANES), f32(4, height, LANES), f32(4, height, LANES),
        f32(32, nz * LANES), f32(3, LANES, LANES),
        dma((7,)), dma((31,)), dma((31,)), dma((2,)), dma((nz,)), dma((nz,)), dma((nz,)), dma((3,)), dma((4,)), dma((2,)),
    ]
    return pl.pallas_call(
        functools.partial(kernel, ng, nz, count),
        out_shape=(jax.ShapeDtypeStruct(fw.shape, F32), jax.ShapeDtypeStruct(tile, F32)),
        in_specs=[anywhere] * 5,
        out_specs=(anywhere, anywhere),
        scratch_shapes=scratch,
        compiler_params=pltpu.CompilerParams(collective_id=0, has_side_effects=True,
                                             vmem_limit_bytes=60 * 1024 * 1024),
        name="step",
    )(spk, w, hb, fw, fb)


def hand_over(w_in, b_in, w_out, b_out, w, b, sem):
    loads = [pltpu.make_async_copy(w_in, w, sem.at[0]), pltpu.make_async_copy(b_in, b, sem.at[1])]
    stores = [pltpu.make_async_copy(w, w_out, sem.at[2]), pltpu.make_async_copy(b, b_out, sem.at[3])]
    for load in loads:
        load.start()
    for load, store in zip(loads, stores):
        load.wait()
        store.start()
    for store in stores:
        store.wait()


def final(w, b):
    anywhere = pl.BlockSpec(memory_space=pl.ANY)
    return pl.pallas_call(
        hand_over,
        out_shape=(jax.ShapeDtypeStruct(w.shape, F32), jax.ShapeDtypeStruct(b.shape, F32)),
        in_specs=[anywhere, anywhere],
        out_specs=(anywhere, anywhere),
        scratch_shapes=[pltpu.VMEM(w.shape, F32), pltpu.VMEM(b.shape, F32), pltpu.SemaphoreType.DMA((4,))],
        compiler_params=pltpu.CompilerParams(vmem_limit_bytes=60 * 1024 * 1024),
        name="hand_over",
    )(w, b)


def solution(mesh):
    ng, ns = mesh.shape["grp"], mesh.shape["smp"]
    nz = ns // 4

    def body(spk, w, hb, fw, fb):
        count = spk.shape[1] * ns
        tile = (8, LANES)
        pad = 8 * LANES - hb.shape[0]
        hb, fb = (jnp.pad(v, (0, pad)).reshape(tile) for v in (hb, fb))
        out_w, out_b = final(*call(ng, nz, count, spk, w, hb, fw, fb))
        return out_w, out_b.reshape(-1)[: nz * LANES]

    return jax.shard_map(body, mesh=mesh,
                         in_specs=(P(None, "smp"), P(None, "grp"), P("grp"), P("smp", "grp"), P("grp")),
                         out_specs=(P("smp", "grp"), P("grp")), check_vma=False)
```

```python
import functools

import jax
import jax.numpy as jnp
from jax import lax
from jax.experimental import pallas as pl
from jax.experimental.pallas import tpu as pltpu
from jax.sharding import PartitionSpec as P

MESH = pl.DeviceIdType.MESH
LAMBDA = 0.01
F32 = jnp.float32
BF16 = jnp.bfloat16
LANES = 128


def split(x):
    hi = x.astype(BF16)
    return hi, (x - hi.astype(F32)).astype(BF16)


def folded(x):
    rows, cols = x.shape
    tiles = [x[r : r + 8, k : k + LANES] for r in range(0, rows, 8) for k in range(0, cols, LANES)]
    return functools.reduce(lambda a, b: a + b, tiles)


def total(x):
    return jnp.sum(jnp.sum(x, axis=0, keepdims=True), axis=1, keepdims=True)


def row_of(x):
    return jnp.sum(x, axis=0, keepdims=True)


def added(parts):
    return functools.reduce(lambda a, b: a + b, parts)


def kernel(ng, nz, count, spk_h, w_h, hb_h, fw_h, fb_h, out_w_h, out_b_h,
           spk, fw, hb, fb, out_w, out_b, pk, wv, wt, fc, ft, sgn, hid, ch,
           vbuf, v1, v2, v3, v2s, v3s, w1, w2, w2s,
           p1s, p1, p2s, p2, p3s, p3, n1s, n1, n2s, n2, b1s, b1, b2s, b2, m1s, m1, x2s, x2, x3s, x3, w3s, w3,
           gb, gi, rs_s, rs_r, gall, gown, cols,
           local_sem, send, recv, near_sem, fa_sem, out_sem, on_sem, fx_sem, rs_sem, ag_sem):
    ns = 4 * nz
    tok = spk.shape[1]
    tiles = tok // LANES
    height = 32 * nz
    s = lax.axis_index("smp")
    g = lax.axis_index("grp")
    xh = s // (2 * nz)
    z = (s // 2) % nz
    c = s % 2
    q_me = 2 * xh + c
    q_core = 2 * xh + 1 - c
    q_x = 2 * (1 - xh) + c
    q_far = 2 * (1 - xh) + 1 - c
    core = s + 1 - 2 * c
    across = s + (2 * nz) * (1 - 2 * xh)

    def z_index(k):
        return 2 * nz * xh + 2 * k + c

    def remote(src, dst, ssem, rsem, dev):
        return pltpu.make_async_remote_copy(src_ref=src, dst_ref=dst, send_sem=ssem, recv_sem=rsem,
                                            device_id=dev, device_id_type=MESH)

    def peers(n, me, act, low=1, high=None):
        def step(j, carry):
            act(lax.rem(me + j, n))
            return carry
        lax.fori_loop(low, n if high is None else high, step, 0)

    def all_of(region, number, sent):
        move = remote(region, region, send.at[number], recv.at[number], {"smp": core})
        move.wait_send() if sent else move.wait_recv()

    class Exchange:
        def __init__(self, n, me, dev, src, dst, number, region):
            self.n, self.me, self.dev, self.src, self.dst = n, me, dev, src, dst
            self.number, self.region = number, region

        def start(self):
            peers(self.n, self.me, lambda p: remote(self.src(p), self.dst(self.me), send.at[self.number],
                                                    recv.at[self.number], self.dev(p)).start())

        def wait(self):
            all_of(self.region, self.number, False)

        def drain(self):
            all_of(self.region, self.number, True)

    def rows_of(buf, n, dst):
        return buf.at[pl.ds(0, n - 1)] if dst is None else dst

    def over_z(src, buf, number, dst=None, region=None):
        return Exchange(nz, z, lambda p: {"smp": z_index(p)}, src, dst or (lambda k: buf.at[k]), number,
                        rows_of(buf, nz, region))

    def over_grp(src, buf, number):
        return Exchange(ng, g, lambda p: {"grp": p}, src, lambda k: buf.at[k], number, rows_of(buf, ng, None))

    def quad_index(q):
        return 2 * nz * (q // 2) + 2 * z + q % 2

    def over_quad(src, buf, number):
        return Exchange(4, q_me, lambda p: {"smp": quad_index(p)}, src, lambda k: buf.at[k], number,
                        rows_of(buf, 4, None))

    plane = 4 * g + q_me
    quads = [quad_index(lax.rem(q_me + d, 4)) for d in range(4)]

    def over_all(do):
        for index in quads[1:]:
            do({"grp": g, "smp": index})

        def step(j, carry):
            h = lax.rem(g + j, ng)
            for index in quads:
                do({"grp": h, "smp": index})
            return carry
        lax.fori_loop(1, ng, step, 0)

    class Plane:
        def __init__(self, src, buf, number):
            self.src, self.buf, self.number = src, buf, number
            self.region = buf.at[pl.ds(0, 4 * ng - 1)]

        def start(self):
            over_all(lambda dev: remote(self.src, self.buf.at[plane], send.at[self.number], recv.at[self.number],
                                        dev).start())

        def wait(self):
            all_of(self.region, self.number, False)

        def drain(self):
            all_of(self.region, self.number, True)

    def lane(k, width=LANES):
        return pl.ds(k * width if isinstance(k, int) else pl.multiple_of(k * width, width), width)

    def block(k, size=32):
        return pl.ds(pl.multiple_of(k * size, size), size)

    loads = [pltpu.make_async_copy(a, b, local_sem.at[i]) for i, (a, b) in enumerate(
        ((spk_h, spk), (w_h.at[:, lane(z)], wv), (hb_h, hb), (fb_h, fb), (fw_h, fw)))]
    barrier = pltpu.get_barrier_semaphore()
    peers(nz, z, lambda p: pl.semaphore_signal(barrier, inc=1, device_id={"smp": z_index(p)}, device_id_type=MESH))
    loads[0].start()
    over_all(lambda dev: pl.semaphore_signal(barrier, inc=1, device_id=dev, device_id_type=MESH))
    for load in loads[1:]:
        load.start()

    ex_v1 = over_grp(lambda p: vbuf.at[p], v1, 1)
    ex_v2 = over_z(lambda p: v2s, v2, 2)
    ex_v3 = over_grp(lambda p: v3s, v3, 3)
    ex_w1 = over_grp(lambda p: vbuf.at[nz + p], w1, 4)
    ex_w2 = over_z(lambda p: w2s, w2, 5)
    ex_w3 = Plane(w3s, w3, 6)
    ex_p1 = over_grp(lambda p: p1s, p1, 7)
    ex_p2 = over_z(lambda p: p2s, p2, 8)
    ex_p3 = over_quad(lambda p: p3s, p3, 9)
    ex_n1 = Plane(n1s, n1, 10)
    ex_n2 = over_z(lambda p: n2s, n2, 11)
    ex_b1 = over_quad(lambda p: b1s, b1, 12)
    ex_b2 = over_z(lambda p: b2s, b2, 13)
    ex_m1 = Plane(m1s, m1, 29)
    ex_x2 = Plane(x2s, x2, 14)
    ex_x3 = over_z(lambda p: x3s, x3, 30)
    ex_gz = over_z(lambda p: gall.at[q_me, block(p)], gown, 15, lambda k: gown.at[:, lane(k)],
                   gown.at[:, pl.ds(0, LANES * (nz - 1))])

    def gather(buf, first, sems):
        to_core = remote(buf.at[q_me], buf.at[q_me], send.at[first], sems.at[0], {"smp": core})
        to_x = remote(buf.at[q_me], buf.at[q_me], send.at[first + 1], sems.at[1], {"smp": across})
        on = remote(buf.at[q_x], buf.at[q_x], send.at[first + 2], sems.at[2], {"smp": core})
        from_core = remote(buf.at[q_core], buf.at[q_core], send.at[first], sems.at[0], {"smp": core})
        from_x = remote(buf.at[q_x], buf.at[q_x], send.at[first + 1], sems.at[1], {"smp": across})
        from_on = remote(buf.at[q_far], buf.at[q_far], send.at[first + 2], sems.at[2], {"smp": core})
        return to_core, to_x, on, from_core, from_x, from_on

    fx = gather(fc, 16, fx_sem)

    piece = tok // ng
    up, down = lax.rem(z + 1, nz), lax.rem(z + nz - 1, nz)
    near = [remote(spk, pk.at[z], send.at[22 + i], near_sem.at[i], {"smp": z_index(k)})
            for i, k in enumerate((up, down))]
    from_near = [remote(spk, pk.at[k], send.at[22 + i], near_sem.at[i], {"smp": z_index(up)})
                 for i, k in enumerate((down, up))]

    def force_out(k):
        return remote(fw.at[:, lane(k)], fc.at[q_me, block(z)], send.at[0], fa_sem.at[z], {"smp": z_index(k)})

    def force_in(k):
        part = fc.at[q_me, block(k)]
        return remote(part, part, send.at[0], fa_sem.at[k], {"smp": z_index(k)})

    def force_on(k):
        part = fc.at[q_me, block(k)]
        remote(part, part, send.at[17], fx_sem.at[1], {"smp": across}).start()
        remote(part, part, send.at[16], fx_sem.at[0], {"smp": core}).start()

    def far_out(k):
        return remote(spk.at[:, lane(g, piece)], pk.at[z, :, lane(g, piece)], send.at[24], out_sem.at[z],
                      {"smp": z_index(k)})

    def far_first(k):
        part = pk.at[k, :, lane(g, piece)]
        return remote(part, part, send.at[24], out_sem.at[k], {"smp": z_index(k)})

    def far_on(k, h):
        part = pk.at[k, :, lane(g, piece)]
        return remote(part, part, send.at[25], on_sem.at[k], {"grp": h})

    def far_rest(k):
        part = pk.at[k, :, pl.ds(0, piece * (ng - 1))]
        return remote(part, part, send.at[25], on_sem.at[k], {"smp": core})

    bit = jnp.left_shift(jnp.int32(1), lax.broadcasted_iota(jnp.int32, (16, tok), 0)).astype(jnp.int16)

    def unpack(words, j):
        for xq in range(2):
            for cq in range(2):
                for k in range(nz):
                    row = words[pl.ds(2 * nz * xq + 2 * k + cq, 1), :]
                    at = ((2 * xq + cq) * nz + k) * 32
                    for half in range(2):
                        word = jnp.right_shift(row, 16 * half) if half else row
                        word = jnp.broadcast_to(word, (16, tok)).astype(jnp.int16)
                        sgn[pl.ds(at + 16 * half, 16), lane(j, tok)] = jnp.where(
                            jnp.bitwise_and(word, bit) != 0, BF16(1), BF16(-1))

    def hidden(j):
        pre = jnp.dot(wt[...], sgn[:, lane(j, tok)], preferred_element_type=F32)
        for r in range(tiles):
            part = pre[:, r * LANES : (r + 1) * LANES] + cols[0]
            hid[:, lane(j * tiles + r)] = jnp.tanh(part)

    loads[0].wait()
    unpack(spk, 0)
    loads[1].wait()
    loads[2].wait()
    loads[3].wait()
    cols[0] = jnp.broadcast_to(hb[pl.ds(z, 1), :], (LANES, LANES)).T
    cols[1] = jnp.broadcast_to(fb[pl.ds(z, 1), :], (LANES, LANES)).T
    for q in range(4):
        parts = [wv[pl.ds(32 * (2 * nz * (q // 2) + 2 * k + q % 2), 32), :] for k in range(nz)]
        wt[:, q * height : (q + 1) * height] = jnp.concatenate(parts, axis=0).astype(F32).T.astype(BF16)
    loads[4].wait()
    n1s[...] = row_of(folded(fw[...] * fw[...]) + folded(fb[...] * fb[...]) * F32(1.0 / ns))

    pl.semaphore_wait(barrier, nz - 1 + 4 * ng - 1)
    peers(nz, z, lambda k: force_out(k).start())
    peers(nz, z, lambda k: far_out(k).start(), 2, nz - 1)
    for move in near:
        move.start()
    fc[q_me, block(z), :] = fw[:, lane(z)]
    hidden(0)
    ex_n1.start()
    n1[plane] = n1s[...]
    def shard(j):
        d = (j + 1) // 2
        return lax.rem(z + (2 * (j % 2) - 1) * d + nz, nz)

    def each(low, high, act):
        def step(j, carry):
            act(j)
            return carry
        lax.fori_loop(low, high, step, 0)

    once = (s + ns) // ns

    force_on(z)

    def force_pass(j):
        force_in(shard(j)).wait_recv()
        force_on(shard(j))

    each(1, nz, force_pass)

    def pass_on(j):
        k = shard(j)
        far_first(k).wait_recv()
        peers(ng, g, lambda h: far_on(k, h).start())

    each(3, nz, pass_on)

    def transposed(buf, q):
        hi, lo = split(buf[q].T)
        ft[:LANES, lane(q, height)] = hi
        ft[LANES:, lane(q, height)] = lo

    def values(slot, wide, base, col, rows, more=False):
        span = pl.ds(slot * tok, wide * tok)
        res = jnp.dot(ft[:, rows], sgn[rows, span], preferred_element_type=F32)
        for n in range(wide):
            k = shard(slot + n)
            for r in range(tiles):
                at = (n * tiles + r) * LANES
                both = res[:LANES, at : at + LANES] + res[LANES:, at : at + LANES]
                if col is not None:
                    both = both + cols[col]
                got = row_of(both * hid[:, lane((slot + n) * tiles + r)])
                to = (base + k, pl.ds(r, 1), slice(None))
                vbuf[to] = vbuf[to] + got if more else got

    transposed(fc, q_me)
    fx[3].wait_recv()
    transposed(fc, q_core)
    for i in (1, 0):
        from_near[i].wait_recv()
        unpack(pk.at[(down, up)[i]], 2 - i)
        hidden(2 - i)
    def arrive(j):
        k = shard(j)
        far_rest(k).wait_recv()
        unpack(pk.at[k], j)
        hidden(j)

    fx[4].wait_recv()
    fx[2].start()
    transposed(fc, q_x)
    early = 3 if nz == 4 else 5
    each(3, early, arrive)
    fx[5].wait_recv()
    transposed(fc, q_far)
    every = pl.ds(0, 4 * height)
    values(0, 3, 0, 1, every)
    for j in range(early, nz):
        far_rest(shard(j)).wait_recv()

    def overlap(_):
        for j in range(early, nz):
            unpack(pk.at[shard(j)], j)
            if j == early and early > 3:
                values(3, early - 3, 0, 1, every)
            hidden(j)

    each(0, once, overlap)
    values(early, nz - early, 0, 1, every)

    ex_v1.start()
    p1s[...] = row_of(added([vbuf[k] for k in range(nz)]))
    ex_p1.start()
    v1[g] = vbuf[g]
    p1[g] = p1s[...]
    ex_n1.wait()
    n2s[...] = added([n1[k] for k in range(4 * ng)])
    ex_n2.start()
    n2[z] = n2s[...]
    ex_v1.wait()
    v2s[...] = added([v1[k] for k in range(ng)])
    ex_v2.start()
    ex_p1.wait()
    p2s[...] = added([p1[k] for k in range(ng)])
    ex_p2.start()
    v2[z] = v2s[...]
    p2[z] = p2s[...]
    peers(nz, z, lambda k: force_out(k).wait_send())
    ex_v1.drain()
    ex_p1.drain()
    ex_n1.drain()
    for move in near:
        move.wait_send()
    peers(nz, z, lambda k: far_out(k).wait_send(), 2, nz - 1)
    ex_v2.wait()
    v3s[...] = added([v2[k] for k in range(nz)])
    ex_v3.start()
    ex_p2.wait()
    p3s[...] = added([p2[k] for k in range(nz)])
    ex_p3.start()
    v3[g] = v3s[...]
    p3[q_me] = p3s[...]
    ex_v2.drain()
    ex_p2.drain()
    peers(nz, z, lambda k: far_rest(k).wait_send(), 2, nz - 1)
    ex_v3.wait()
    ex_p3.wait()
    inv = F32(1.0 / count)
    mean = total(added([p3[k] for k in range(4)])) * inv
    mine = (c, 2 + c)
    other = (1 - c, 3 - c)

    def first_rows(_):
        bias = jnp.zeros((LANES, LANES), F32)
        sums = [None, None]
        for j in range(nz):
            own = v3[shard(j)] - mean
            for r in range(tiles):
                at = (j * tiles + r) * LANES
                prod = hid[:, at : at + LANES] * own[r : r + 1, :]
                hi, lo = split(prod)
                ch[:LANES, at : at + LANES] = hi
                ch[LANES:, at : at + LANES] = lo
                bias = bias + prod
            span = slice(j * tok, (j + 1) * tok)
            res = lax.dot_general(sgn[block(other[0], height), span], ch[:, span],
                                  (((1,), (1,)), ((), ())), preferred_element_type=F32)
            sums[j % 2] = res if j < 2 else sums[j % 2] + res
        res = sums[0] + sums[1]
        gi[other[0]] = res[:, :LANES] + res[:, LANES:]
        gb[...] = bias

    each(0, once, first_rows)

    def image(q):
        def run(_):
            res = lax.dot_general(sgn[block(q, height), :], ch[...], (((1,), (1,)), ((), ())),
                                  preferred_element_type=F32)
            gi[q] = res[:, :LANES] + res[:, LANES:]
        each(0, once, run)

    to_core = [remote(gi.at[other[i]], rs_r.at[i], send.at[26 + i], rs_sem.at[i], {"smp": core}) for i in range(2)]
    to_x = [remote(rs_s.at[i], rs_r.at[2 + i], send.at[19 + i], rs_sem.at[2 + i], {"smp": across}) for i in range(2)]
    share = [remote(gall.at[mine[i]], gall.at[mine[i]], send.at[21 + 7 * i], ag_sem.at[i], {"smp": core})
             for i in range(2)]
    shared = [remote(gall.at[other[i]], gall.at[other[i]], send.at[21 + 7 * i], ag_sem.at[i], {"smp": core})
              for i in range(2)]
    to_core[0].start()
    b1s[...] = row_of(gb[...].T)
    off = v3s[...] - mean
    m1s[...] = row_of(off * off)
    ex_b1.start()
    b1[q_me] = b1s[...]
    image(mine[0])
    to_core[0].wait_recv()
    rs_s[0] = gi[mine[0]] + rs_r[0]
    to_x[0].start()
    ex_m1.start()
    m1[plane] = m1s[...]
    image(other[1])
    to_core[1].start()
    image(mine[1])
    to_core[1].wait_recv()
    rs_s[1] = gi[mine[1]] + rs_r[1]
    to_x[1].start()
    ex_v3.drain()
    ex_p3.drain()
    ex_n2.wait()
    ex_n2.drain()
    norm0 = total(added([n2[k] for k in range(nz)]))
    ex_b1.wait()
    b2s[...] = added([b1[k] for k in range(4)])
    ex_b2.start()
    b2[z] = b2s[...]
    cols[2] = jnp.broadcast_to(b2s[...], (LANES, LANES)).T
    ex_b1.drain()

    def quarter(q, first=False):
        transposed(gall, q)
        each(0, once, lambda i: values(0, nz, nz, 2 if first else None, block(q, height), not first))

    to_x[0].wait_recv()
    gall[mine[0]] = rs_s[0] + rs_r[2]
    share[0].start()
    quarter(mine[0], True)
    shared[0].wait_recv()
    quarter(other[0])
    ex_b2.wait()
    ex_m1.wait()
    for k in range(nz):
        gb[pl.ds(k, 1), :] = b2[k]
    if nz < 8:
        gb[nz:8, :] = jnp.zeros((8 - nz, LANES), F32)
    image_b = gb[:8, :]
    curvature = total(added([m1[k] for k in range(4 * ng)])) * inv + F32(LAMBDA) * norm0
    alpha0 = norm0 / curvature
    to_x[1].wait_recv()
    gall[mine[1]] = rs_s[1] + rs_r[3]
    share[1].start()
    ex_gz.start()
    gown[:, lane(z)] = gall[q_me, block(z), :]

    res_b = fb[...] - alpha0 * (image_b * inv + F32(LAMBDA) * fb[...])
    own_f = fc[q_me]
    res_w = own_f - alpha0 * (gall[q_me] * inv + F32(LAMBDA) * own_f)
    x2s[0:1] = row_of(folded(res_w * res_w) + res_b * res_b * F32(1.0 / ns))
    x2s[1:2] = row_of(folded(res_w * own_f) + res_b * fb[...] * F32(1.0 / ns))
    ex_x2.start()
    x2[plane] = x2s[...]
    quarter(mine[1])
    shared[1].wait_recv()
    quarter(other[1])

    ex_w1.start()
    w1[g] = vbuf[nz + g]
    ex_x2.wait()
    x3s[...] = added([x2[k] for k in range(4 * ng)])
    ex_x3.start()
    x3[z] = x3s[...]
    for move in (*fx[:3], *to_core, *to_x, *share):
        move.wait_send()
    for ex in (ex_m1, ex_b2, ex_gz):
        ex.drain()
    ex_gz.wait()
    ex_w1.wait()
    w2s[...] = added([w1[k] for k in range(ng)])
    ex_w2.start()
    w2[z] = w2s[...]
    ex_w1.drain()
    ex_x2.drain()
    ex_x3.wait()
    ex_x3.drain()
    sums = added([x3[k] for k in range(nz)])
    norm1 = total(sums[0:1])
    cross = total(sums[1:2])
    beta = norm1 / norm0
    scale_f = F32(1.0) - alpha0 * F32(LAMBDA) + beta
    norm_d = norm1 + F32(2.0) * beta * cross + beta * beta * norm0
    ex_w2.wait()
    mixed = scale_f * off - (alpha0 * inv) * added([w2[k] for k in range(nz)])
    here = total(mixed)
    spread = mixed - here * F32(1.0 / tok)
    w3s[0:1] = jnp.broadcast_to(here, (1, LANES))
    w3s[1:2] = row_of(spread * spread)
    ex_w3.start()
    w3[plane] = w3s[...]
    ex_w2.drain()
    ex_w3.wait()
    shards = [w3[k, 0:1, :] for k in range(4 * ng)]
    mean1 = added(shards) * inv
    between = row_of(jnp.zeros((1, LANES), F32))
    for one in shards:
        gap = one * F32(1.0 / tok) - mean1
        between += gap * gap
    within = total(added([w3[k, 1:2, :] for k in range(4 * ng)]))
    square = within + between[:, 0:1] * F32(tok)
    curvature = square * inv + F32(LAMBDA) * norm_d
    alpha1 = norm1 / curvature
    factor_f = alpha0 + alpha1 * scale_f
    factor_g = alpha1 * alpha0 * inv
    out_w[...] = factor_f * fw[...] - factor_g * gown[...]
    out_b[...] = factor_f * fb[...] - factor_g * image_b
    stores = [pltpu.make_async_copy(a, b, local_sem.at[5 + i]) for i, (a, b) in enumerate(
        ((out_w, out_w_h), (out_b, out_b_h)))]
    for store in stores:
        store.start()
    ex_w3.drain()
    for store in stores:
        store.wait()


def call(ng, nz, count, spk, w, hb, fw, fb):
    ns = 4 * nz
    tok = spk.shape[1]
    words, height = spk.shape[0], 32 * nz
    nv = 32 * words
    tile = (8, LANES)
    dma = pltpu.SemaphoreType.DMA
    anywhere = pl.BlockSpec(memory_space=pl.ANY)

    def f32(*shape):
        return pltpu.VMEM(shape, F32)

    scratch = [
        pltpu.VMEM((words, tok), jnp.int32), f32(*fw.shape), f32(*tile), f32(*tile), f32(*fw.shape), f32(*tile),
        pltpu.VMEM((nz, words, tok), jnp.int32),
        pltpu.VMEM((nv, LANES), BF16),
        pltpu.VMEM((LANES, nv), BF16),
        f32(4, height, LANES),
        pltpu.VMEM((2 * LANES, nv), BF16),
        pltpu.VMEM((nv, nz * tok), BF16),
        f32(LANES, nz * tok),
        pltpu.VMEM((2 * LANES, nz * tok), BF16),
        f32(2 * nz, *tile), f32(ng, *tile), f32(nz, *tile), f32(ng, *tile), f32(*tile), f32(*tile),
        f32(ng, *tile), f32(nz, *tile), f32(*tile),
        f32(1, LANES), f32(ng, 1, LANES), f32(1, LANES), f32(nz, 1, LANES), f32(1, LANES), f32(4, 1, LANES),
        f32(1, LANES), f32(4 * ng, 1, LANES), f32(1, LANES), f32(nz, 1, LANES),
        f32(1, LANES), f32(4, 1, LANES), f32(1, LANES), f32(nz, 1, LANES), f32(1, LANES), f32(4 * ng, 1, LANES),
        f32(2, LANES), f32(4 * ng, 2, LANES), f32(2, LANES), f32(nz, 2, LANES), f32(2, LANES), f32(4 * ng, 2, LANES),
        f32(LANES, LANES), f32(4, height, LANES), f32(2, height, LANES), f32(4, height, LANES), f32(4, height, LANES),
        f32(32, nz * LANES), f32(3, LANES, LANES),
        dma((7,)), dma((31,)), dma((31,)), dma((2,)), dma((nz,)), dma((nz,)), dma((nz,)), dma((3,)), dma((4,)), dma((2,)),
    ]
    return pl.pallas_call(
        functools.partial(kernel, ng, nz, count),
        out_shape=(jax.ShapeDtypeStruct(fw.shape, F32), jax.ShapeDtypeStruct(tile, F32)),
        in_specs=[anywhere] * 5,
        out_specs=(anywhere, anywhere),
        scratch_shapes=scratch,
        compiler_params=pltpu.CompilerParams(collective_id=0, has_side_effects=True,
                                             vmem_limit_bytes=60 * 1024 * 1024),
        name="step",
    )(spk, w, hb, fw, fb)


def hand_over(w_in, b_in, w_out, b_out, w, b, sem):
    loads = [pltpu.make_async_copy(w_in, w, sem.at[0]), pltpu.make_async_copy(b_in, b, sem.at[1])]
    stores = [pltpu.make_async_copy(w, w_out, sem.at[2]), pltpu.make_async_copy(b, b_out, sem.at[3])]
    for load in loads:
        load.start()
    for load, store in zip(loads, stores):
        load.wait()
        store.start()
    for store in stores:
        store.wait()


def final(w, b):
    anywhere = pl.BlockSpec(memory_space=pl.ANY)
    return pl.pallas_call(
        hand_over,
        out_shape=(jax.ShapeDtypeStruct(w.shape, F32), jax.ShapeDtypeStruct(b.shape, F32)),
        in_specs=[anywhere, anywhere],
        out_specs=(anywhere, anywhere),
        scratch_shapes=[pltpu.VMEM(w.shape, F32), pltpu.VMEM(b.shape, F32), pltpu.SemaphoreType.DMA((4,))],
        compiler_params=pltpu.CompilerParams(vmem_limit_bytes=60 * 1024 * 1024),
        name="hand_over",
    )(w, b)


def solution(mesh):
    ng, ns = mesh.shape["grp"], mesh.shape["smp"]
    nz = ns // 4

    def body(spk, w, hb, fw, fb):
        count = spk.shape[1] * ns
        tile = (8, LANES)
        pad = 8 * LANES - hb.shape[0]
        hb, fb = (jnp.pad(v, (0, pad)).reshape(tile) for v in (hb, fb))
        out_w, out_b = final(*call(ng, nz, count, spk, w, hb, fw, fb))
        return out_w, out_b.reshape(-1)[: nz * LANES]

    return jax.shard_map(body, mesh=mesh,
                         in_specs=(P(None, "smp"), P(None, "grp"), P("grp"), P("smp", "grp"), P("grp")),
                         out_specs=(P("smp", "grp"), P("grp")), check_vma=False)
```
